32 devices in a mesh: expert: 4 (over y, core), context: 2 (over x), dp: 4 (over z).
Axes of the slice: x: 2, y: 2, z: 4, core: 2. Of those that a mesh axis runs over, the one named last changes fastest.
Arguments:
- layer_input: bfloat16 [4, 1024, 2048], P('dp', ('expert', 'context')), may hold values from -6 to 6
- output_grad: bfloat16 [4, 1024, 2048], P('dp', ('expert', 'context')), may hold values from -6 to 6
- lengths: int32 [4], P('dp'), may hold values from 256 to 1024, as said below
- attn_routes: int32 [4, 1024, 2], P('dp', ('expert', 'context')), may hold values from 0 to 3, all different within a row; in each aligned block of 128 rows (0 to 127, 128 to 255, ..., all dimensions but the last counted through in order) at most 68 rows name the same one
- ffn_routes: int32 [4, 1024, 2], P('dp', ('expert', 'context')), may hold values from 0 to 3, all different within a row; in each aligned block of 128 rows (0 to 127, 128 to 255, ..., all dimensions but the last counted through in order) at most 68 rows name the same one
- norm1_gain: float32 [2048], replicated, may hold values from 0.1 to 1.9
- norm2_gain: float32 [2048], replicated, may hold values from 0.1 to 1.9
- attn_router: bfloat16 [2048, 4], replicated, may hold values from -0.125 to 0.125
- ffn_router: bfloat16 [2048, 4], replicated, may hold values from -0.125 to 0.125
- w_kv: bfloat16 [2048, 4096], P(('context', 'dp')), may hold values from -0.125 to 0.125
- w_query: bfloat16 [4, 2048, 2048], P('expert', ('context', 'dp')), may hold values from -0.125 to 0.125
- w_out: bfloat16 [4, 2048, 2048], P('expert', ('context', 'dp')), may hold values from -2 to 2
- w_in: bfloat16 [4, 11264, 2048], P('expert', ('context', 'dp')), may hold values from -0.125 to 0.125
- w_down: bfloat16 [4, 5632, 2048], P('expert', ('context', 'dp')), may hold values from -0.078125 to 0.078125
Outputs:
- layer_output: bfloat16 [4, 1024, 2048], P('dp', ('expert', 'context'))
- input_grad: float32 [4, 1024, 2048], P('dp', ('expert', 'context'))
- grad_norm1_gain: float32 [2048], replicated
- grad_norm2_gain: float32 [2048], replicated
- grad_attn_router: float32 [2048, 4], replicated
- grad_ffn_router: float32 [2048, 4], replicated
- grad_w_kv: float32 [2048, 4096], P(('context', 'dp'))
- grad_w_query: float32 [4, 2048, 2048], P('expert', ('context', 'dp'))
- grad_w_out: float32 [4, 2048, 2048], P('expert', ('context', 'dp'))
- grad_w_in: float32 [4, 11264, 2048], P('expert', ('context', 'dp'))
- grad_w_down: float32 [4, 5632, 2048], P('expert', ('context', 'dp'))
The draws below stay inside these ranges and needn't reach their ends.
Inputs may be any that keep to these rules, and one draw needn't show every extreme that they name: Slot s holds one sequence at positions 0 to lengths[s] - 1; the rest is padding. `attn_routes`: the two experts of a position differ; among the 128 positions of one device no expert is named by more than 68. `ffn_routes`: the two experts of a position differ; among the 128 positions of one device no expert is named by more than 68.
All inputs are finite; a program needn't handle non-finite values.
Results may differ from the reference program's by a relative error of at most 0.033.
Values may be sent and summed in bfloat16 or wider, within the bound.
A program may use at most 384 MiB of HBM per device.

```python
import math
import jax
import jax.numpy as jnp
import numpy as np
from jax import lax

D = 2048
HEADS = 16
HEAD_DIM = 128
FF = 5632
TOP = 2
TOK_DEV = 128
EXPERTS = 4
QD = 2048
CAP = 68
SLOT = 1024
SLOTS = 4


def draw_lengths(key, part):
    key_one, key_two = jax.random.split(key)
    picked = jax.random.randint(key_one, (SLOTS,), SLOT // 4, SLOT + 1)
    order = jax.random.permutation(key_two, SLOTS)
    picked = picked.at[order[0]].set(SLOT)
    picked = picked.at[order[1]].set(SLOT // 4)
    return picked.astype(jnp.int32)


def shard_levels(key, extent, cuts, smallest, largest):
    def one(position, shards_of):
        draws = jax.random.uniform(jax.random.fold_in(jax.random.fold_in(key, 6), position), (shards_of,), jnp.float32, smallest / len(cuts), largest / len(cuts))
        return jnp.repeat(jnp.exp(draws), extent[position] // shards_of).reshape((-1,) + (1,) * (len(extent) - position - 1))

    level = one(*cuts[0])
    for cut in cuts[1:]:
        level = level * one(*cut)
    return level


def shared_out(rng, own, number, rows, number_of, top, bound, skew):
    ranking = jax.random.permutation(rng, number_of)
    crowded, usual = portions_of(number_of, rows * top, bound, skew, True), portions_of(number_of, rows * top, bound, skew, False)
    places = jnp.arange(number_of)

    def named(tallies, offset_by):
        used = int((tallies > 0).sum())
        fixed = max(1, used // 4)
        moved = fixed + (places - fixed + offset_by * (used - fixed)) % max(1, number_of - fixed)
        return jnp.zeros((number_of,), jnp.int32).at[ranking[jnp.where(places < fixed, places, moved)]].set(jnp.asarray(tallies, jnp.int32))

    tallies = jnp.where(number % 4 == 0, named(crowded, number // 4), named(usual, number - number // 4 - 1))
    mixed = jax.random.permutation(jax.random.fold_in(own, 3), number_of)
    source_of, taker = mixed[0:number_of // 2 * 2:2], mixed[1:number_of // 2 * 2:2]
    room = jnp.minimum(tallies[source_of] - 1, bound - tallies[taker]) // 2
    room = jnp.where((source_of == ranking[0]) | (taker == ranking[0]) | (tallies[taker] == 0), 0, jnp.maximum(room, 0))
    moved = jax.random.randint(jax.random.fold_in(own, 4), (number_of // 2,), 0, 1 << 20) % (room + 1)
    tallies = tallies.at[source_of].add(-moved).at[taker].add(moved)
    labels = jnp.searchsorted(jnp.cumsum(tallies), jnp.arange(rows * top), side="right").astype(jnp.int32)
    table = labels.reshape(top, rows).T
    table = table[jax.random.permutation(jax.random.fold_in(own, 1), rows)]
    offset_by = jax.random.randint(jax.random.fold_in(own, 2), (rows, 1), 0, top)
    return jnp.take_along_axis(table, (jnp.arange(top)[None, :] + offset_by) % top, axis=1)


def portions_of(number_of, total, limit, skew, full):
    loads = [(1 << 20) // math.isqrt(standing ** skew) + 1 for standing in range(1, number_of + 1)]
    largest = limit if full else min(limit, max(-(-total // number_of), total * loads[0] // sum(loads)))
    least = 1 if total - largest >= number_of - 1 else 0
    holding, spare = [largest] + [least] * (number_of - 1), total - largest - least * (number_of - 1)
    while spare > 0:
        free = [i for i in range(1, number_of) if holding[i] < largest] or [i for i in range(1, number_of) if holding[i] < limit]
        pool, left = sum([loads[i] for i in free]), spare
        for i in free:
            more = min(limit - holding[i], max(1, left * loads[i] // pool), spare)
            holding[i] = holding[i] + more
            spare = spare - more
    return np.array(holding)


def noise(key, shape, deviation, limit, cuts=(), kind=jnp.bfloat16):
    loudness = shard_levels(key, shape, cuts, -0.22, 0.18) if cuts else 1.0
    drawn = jax.random.normal(key, shape, jnp.float32) * deviation * loudness
    return jnp.minimum(jnp.maximum(drawn, -limit), limit).astype(kind)


def setup_inputs(seed: int = 0) -> dict:
    key_of = jax.random.split(jax.random.key(seed), 15)
    layer_input = noise(key_of[0], (SLOTS, SLOT, D), 1.0, 6.0, ((0, 4), (1, 8)))
    output_grad = noise(key_of[1], (SLOTS, SLOT, D), 1.0, 6.0, ((0, 4), (1, 8)))
    lengths = draw_lengths(jax.random.fold_in(key_of[14], 71), 0)
    attn_routes_keys = jax.random.split(jax.random.fold_in(key_of[3], 1), SLOTS * SLOT // TOK_DEV)
    attn_routes_turns = jax.random.permutation(jax.random.fold_in(key_of[3], 3), SLOTS * SLOT // TOK_DEV)
    attn_routes = jax.vmap(lambda own, number: shared_out(jax.random.fold_in(key_of[3], 2), own, number, TOK_DEV, EXPERTS, TOP, CAP, 2))(attn_routes_keys, attn_routes_turns).reshape((SLOTS, SLOT, TOP))
    ffn_routes_keys = jax.random.split(jax.random.fold_in(key_of[4], 1), SLOTS * SLOT // TOK_DEV)
    ffn_routes_turns = jax.random.permutation(jax.random.fold_in(key_of[4], 3), SLOTS * SLOT // TOK_DEV)
    ffn_routes = jax.vmap(lambda own, number: shared_out(jax.random.fold_in(key_of[4], 2), own, number, TOK_DEV, EXPERTS, TOP, CAP, 2))(ffn_routes_keys, ffn_routes_turns).reshape((SLOTS, SLOT, TOP))
    norm1_gain = jnp.clip(1.0 + 0.18 * jax.random.normal(key_of[5], (D,), jnp.float32), 0.1, 1.9)
    norm2_gain = jnp.clip(1.0 + 0.18 * jax.random.normal(key_of[6], (D,), jnp.float32), 0.1, 1.9)
    attn_router = noise(key_of[7], (D, EXPERTS), D ** -0.5, 0.125)
    ffn_router = noise(key_of[8], (D, EXPERTS), D ** -0.5, 0.125)
    w_kv = noise(key_of[9], (D, 2 * QD), D ** -0.5, 0.125, ((0, 8),))
    w_query = noise(key_of[10], (EXPERTS, D, QD), D ** -0.5, 0.125, ((0, 4), (1, 8)))
    w_out = noise(key_of[11], (EXPERTS, QD, D), (max(1, QD // 256)) ** -0.5, 2.0, ((0, 4), (1, 8)))
    w_in = noise(key_of[12], (EXPERTS, 2 * FF, D), D ** -0.5, 0.125, ((0, 4), (1, 8)))
    w_down = noise(key_of[13], (EXPERTS, FF, D), FF ** -0.5, 0.078125, ((0, 4), (1, 8)))
    return {"layer_input": layer_input, "output_grad": output_grad, "lengths": lengths, "attn_routes": attn_routes, "ffn_routes": ffn_routes, "norm1_gain": norm1_gain, "norm2_gain": norm2_gain, "attn_router": attn_router, "ffn_router": ffn_router, "w_kv": w_kv, "w_query": w_query, "w_out": w_out, "w_in": w_in, "w_down": w_down}


EPSILON = 1e-06
PRECISE = lax.Precision.HIGHEST

@jax.custom_vjp
def low(v):
    return lax.optimization_barrier(v.astype(jnp.bfloat16)).astype(jnp.float32)

@jax.custom_vjp
def low_back(v):
    return v

def low_keep(v):
    return (low(v), None)

def low_pass(kept, grad):
    return (grad,)

def back_keep(v):
    return (v, None)

def back_low(kept, grad):
    return (low(grad),)
low.defvjp(low_keep, low_pass)
low_back.defvjp(back_keep, back_low)

def rms_scale(value):
    return lax.rsqrt(lax.optimization_barrier(jnp.mean(value * value, axis=-1, keepdims=True)) + EPSILON)

def mix_gates(logits, routes, live):
    picked = (routes[:, :, None] == jnp.arange(EXPERTS, dtype=jnp.int32)[None, None, :]).astype(jnp.float32)
    chosen = lax.optimization_barrier(jnp.sum(picked * logits[:, None, :], axis=-1))
    highest = lax.optimization_barrier(jnp.max(chosen, axis=-1, keepdims=True))
    exponent = jnp.exp(chosen - highest)
    shares = exponent / lax.optimization_barrier(jnp.sum(exponent, axis=-1, keepdims=True))
    return lax.optimization_barrier(jnp.sum(shares[:, :, None] * picked, axis=1)) * live[:, None]

def attend(query, key_heads, value_heads):
    length = key_heads.shape[0]
    block_len = math.gcd(length, 512)
    key_pos = jnp.arange(length, dtype=jnp.int32)

    def one_block(index):
        first_row = index * block_len
        query_block = lax.dynamic_slice_in_dim(query, first_row, block_len, 1)
        query_pos = first_row + jnp.arange(block_len, dtype=jnp.int32)
        scores = jnp.einsum('eqhd,khd->ehqk', query_block, key_heads, precision=PRECISE) * HEAD_DIM ** (-0.5)
        scores = low_back(scores)
        allowed = key_pos[None, :] <= query_pos[:, None]
        scores = jnp.where(allowed[None, None], scores, -1e+30)
        log_norm = jax.nn.logsumexp(scores, axis=-1, keepdims=True)
        shares = low(jnp.exp(scores - log_norm))
        return jnp.einsum('ehqk,khd->eqhd', shares, value_heads, precision=PRECISE)
    blocks = lax.map(jax.checkpoint(one_block), jnp.arange(length // block_len, dtype=jnp.int32))
    blocks = jnp.transpose(blocks, (1, 0, 2, 3, 4))
    return blocks.reshape(EXPERTS, length, QD)

def layer(x_value, routes_a, routes_f, length, gain_one, gain_two, router_a, router_f, kv_weight, query_weight, out_weight, in_weight, down_weight):
    slots = x_value.shape[0]
    positions = jnp.arange(slots, dtype=jnp.int32)
    live = (positions < length).astype(jnp.float32)
    normed_one = low(x_value * rms_scale(x_value) * gain_one)
    kv_value = low_back(low(jnp.dot(normed_one, kv_weight, precision=PRECISE)))
    key_heads = kv_value[:, :QD].reshape(slots, HEADS, HEAD_DIM)
    value_heads = kv_value[:, QD:].reshape(slots, HEADS, HEAD_DIM)
    gates_a = mix_gates(jnp.dot(normed_one, router_a, precision=PRECISE), routes_a, live)
    copies_one = low_back(jnp.broadcast_to(normed_one[None], (EXPERTS,) + normed_one.shape))
    query = low_back(low(jnp.einsum('esd,edq->esq', copies_one, query_weight, precision=PRECISE)))
    attended = attend(query.reshape(EXPERTS, slots, HEADS, HEAD_DIM), key_heads, value_heads)
    attended = low_back(low(attended))
    branch = low_back(low(jnp.einsum('esq,eqd->esd', attended, out_weight, precision=PRECISE)))
    residual_one = x_value + jnp.einsum('se,esd->sd', gates_a, branch, precision=PRECISE)
    normed_two = low(residual_one * rms_scale(residual_one) * gain_two)
    gates_f = mix_gates(jnp.dot(normed_two, router_f, precision=PRECISE), routes_f, live)
    copies_two = low_back(jnp.broadcast_to(normed_two[None], (EXPERTS,) + normed_two.shape))
    both = jnp.einsum('esd,efd->esf', copies_two, in_weight, precision=PRECISE)
    gate_part = low_back(both[:, :, :FF])
    up_part = low_back(both[:, :, FF:])
    hidden = low(jax.nn.silu(gate_part) * up_part)
    down = low_back(low(jnp.einsum('esf,efd->esd', hidden, down_weight, precision=PRECISE)))
    mixed = jnp.einsum('se,esd->sd', gates_f, down, precision=PRECISE)
    return live[:, None] * (residual_one + mixed)

def reference(layer_input, output_grad, lengths, attn_routes, ffn_routes, norm1_gain, norm2_gain, attn_router, ffn_router, w_kv, w_query, w_out, w_in, w_down):
    params = tuple((p.astype(jnp.float32) for p in (norm1_gain, norm2_gain, attn_router, ffn_router, w_kv, w_query, w_out, w_in, w_down)))

    def one_slot(summed, slot_data):
        slot_x, slot_grad, routes_a, routes_f, length = slot_data

        def layer_of(x_value, *weights):
            return layer(x_value, routes_a, routes_f, length, *weights)
        output, pullback = jax.vjp(layer_of, slot_x.astype(jnp.float32), *params)
        grads = pullback(slot_grad.astype(jnp.float32))
        summed = tuple((a + b for a, b in zip(summed, grads[1:])))
        return (summed, (output.astype(jnp.bfloat16), grads[0]))
    start_sums = tuple((jnp.zeros(p.shape, jnp.float32) for p in params))
    summed, (outputs, input_grads) = lax.scan(one_slot, start_sums, (layer_input, output_grad, attn_routes, ffn_routes, lengths))
    return (outputs, input_grads, summed[0], summed[1], summed[2], summed[3], summed[4], summed[5], summed[6], summed[7], summed[8])
```

```python
import math

import jax
import jax.numpy as jnp
from jax import lax
from jax.experimental import pallas as pl
from jax.experimental.pallas import tpu as pltpu
from jax.sharding import PartitionSpec as P

HEADS = 16
HEAD_DIM = 128
FF = 5632
TOP = 2
QD = 2048


EPSILON = 1e-06
PRECISE = lax.Precision.HIGHEST


def rms_scale(value):
    return lax.rsqrt(jnp.mean(value * value, axis=-1, keepdims=True) + EPSILON)


def norm_back(value, scale, gain, grad_normed):
    weighted = grad_normed * gain
    d_gain = jnp.sum(grad_normed * value * scale, axis=0)
    d_value = scale * weighted - value * scale**3 * jnp.mean(
        weighted * value, axis=-1, keepdims=True
    )
    return (d_value, d_gain)


def weight_fold(left_rows, weight):
    return jnp.dot(
        left_rows,
        lax.all_gather(weight, ("context", "dp"), axis=0, tiled=True),
        preferred_element_type=jnp.float32,
    )


def weight_back(gradient, weight):
    return lax.dot_general(
        gradient,
        lax.all_gather(weight, ("context", "dp"), axis=0, tiled=True),
        (((1,), (1,)), ((), ())),
        preferred_element_type=jnp.float32,
    )


def weight_grad(left_rows, gradient):
    return lax.psum_scatter(
        lax.dot_general(
            left_rows, gradient, (((0,), (0,)), ((), ())), preferred_element_type=jnp.float32
        ).astype(jnp.bfloat16),
        ("context", "dp"),
        scatter_dimension=0,
        tiled=True,
    ).astype(jnp.float32)


def unit_forward(left_rows, weight):
    return lax.dot_general(
        left_rows,
        lax.all_gather(weight, ("context", "dp"), axis=0, tiled=True),
        (((1,), (1,)), ((), ())),
        preferred_element_type=jnp.float32,
    )


def unit_backward(gradient, weight):
    return jnp.dot(
        gradient,
        lax.all_gather(weight, ("context", "dp"), axis=0, tiled=True),
        preferred_element_type=jnp.float32,
    )


def unit_grad(gradient, left_rows):
    return lax.psum_scatter(
        lax.dot_general(
            gradient, left_rows, (((0,), (0,)), ((), ())), preferred_element_type=jnp.float32
        ).astype(jnp.bfloat16),
        ("context", "dp"),
        scatter_dimension=0,
        tiled=True,
    ).astype(jnp.float32)


def to_owner(slot_rows):
    return lax.all_to_all(slot_rows, "expert", split_axis=0, concat_axis=0, tiled=True)


def to_home(slot_rows):
    return lax.all_to_all(slot_rows, "expert", split_axis=0, concat_axis=0, tiled=True)


def pair_gates(logits, routes, live, experts):
    picked = (routes[:, :, None] == jnp.arange(experts, dtype=jnp.int32)[None, None, :]).astype(
        jnp.float32
    )
    chosen = jnp.sum(picked * logits[:, None, :], axis=-1)
    highest = jnp.max(chosen, axis=-1, keepdims=True)
    exponent = jnp.exp(chosen - highest)
    return (exponent / jnp.sum(exponent, axis=-1, keepdims=True) * live[:, None], picked)


def logit_grad(shares, picked, pair_grad):
    mean_grad = jnp.sum(shares * pair_grad, axis=-1, keepdims=True)
    return jnp.sum((shares * (pair_grad - mean_grad))[:, :, None] * picked, axis=1)


def route_table(routes, live_int, experts, capacity):
    owners = (routes[:, :, None] == jnp.arange(experts, dtype=jnp.int32)[None, None, :]).astype(
        jnp.int32
    )
    owners = owners * live_int[:, None, None]
    used_slots = jnp.sum(owners, axis=1)
    before = jnp.cumsum(used_slots, axis=0) - used_slots
    slot_rank = jnp.sum(before[:, None, :] * owners, axis=-1)
    target = routes * capacity + slot_rank
    slot_hits = (
        target[:, :, None] == jnp.arange(experts * capacity, dtype=jnp.int32)[None, None, :]
    ).astype(jnp.int32)
    return slot_hits * live_int[:, None, None]


def dispatch(table_low, token_rows, experts, capacity):
    sent = jnp.einsum("tkr,td->rd", table_low, token_rows, preferred_element_type=jnp.float32)
    return sent.astype(jnp.bfloat16).reshape(experts, capacity, token_rows.shape[1])


def collect_pairs(table_low, received):
    flat = received.reshape(-1, received.shape[-1])
    return jnp.einsum("tkr,rd->tkd", table_low, flat, preferred_element_type=jnp.float32)


def collect_sum(table_low, received):
    flat = received.reshape(-1, received.shape[-1])
    return jnp.einsum("tkr,rd->td", table_low, flat, preferred_element_type=jnp.float32)


def spread_back(table_int, shares, gradient, experts, capacity):
    weighted = shares[:, :, None] * gradient[:, None, :]
    sent = jnp.einsum("tkr,tkd->rd", table_int.astype(jnp.float32), weighted, precision=PRECISE)
    return sent.astype(jnp.bfloat16).reshape(experts, capacity, gradient.shape[1])


def masked_scores(query_heads, key_heads, query_pos, key_pos):
    scores = jnp.einsum(
        "rhd,khd->hrk", query_heads, key_heads, preferred_element_type=jnp.float32
    ) * HEAD_DIM ** (-0.5)
    return (scores, key_pos[None, None, :] <= query_pos[None, :, None])


def key_scan(shard_piece, block_step, carried):
    piece_len = shard_piece.shape[0]
    block_len = math.gcd(piece_len, 512)
    blocks = shard_piece.reshape(piece_len // block_len, block_len, shard_piece.shape[1])
    firsts = jnp.arange(piece_len // block_len, dtype=jnp.int32) * block_len

    def key_one_block(carry_in, element):
        block_rows, first_key = element
        key_heads = block_rows[:, :QD].reshape(block_len, HEADS, HEAD_DIM)
        value_heads = block_rows[:, QD:].reshape(block_len, HEADS, HEAD_DIM)
        key_pos = first_key + jnp.arange(block_len, dtype=jnp.int32)
        return (block_step(carry_in, key_heads, value_heads, key_pos), None)

    carried, _ = lax.scan(key_one_block, carried, (blocks, firsts))
    return carried


def key_fold(kv_rows, block_step, zeros_init):
    return key_scan(
        lax.all_gather(kv_rows, ("expert", "context"), axis=0, tiled=True), block_step, zeros_init
    )


def gathered_weights(
    layer_input,
    output_grad,
    lengths,
    attn_routes,
    ffn_routes,
    norm1_gain,
    norm2_gain,
    attn_router,
    ffn_router,
    w_kv,
    w_query,
    w_out,
    w_in,
    w_down,
):
    tokens = layer_input.shape[1]
    width = layer_input.shape[2]
    experts = lax.axis_size("expert")
    capacity = tokens * TOP // experts + tokens // 32
    row_count = experts * capacity
    position = lax.axis_index(("expert", "context")) * tokens + jnp.arange(tokens, dtype=jnp.int32)
    live_int = (position < lengths[0]).astype(jnp.int32)
    live = live_int.astype(jnp.float32)
    x_float = layer_input[0].astype(jnp.float32)
    scale_one = rms_scale(x_float)
    normed_one = (x_float * scale_one * norm1_gain).astype(jnp.bfloat16)
    kv_rows = weight_fold(normed_one, w_kv).astype(jnp.bfloat16)
    shares_a, picked_a = pair_gates(
        jnp.dot(normed_one, attn_router, preferred_element_type=jnp.float32),
        attn_routes[0],
        live,
        experts,
    )
    table_a = route_table(attn_routes[0], live_int, experts, capacity)
    low_table_a = table_a.astype(jnp.bfloat16)
    send_rows = dispatch(low_table_a, normed_one, experts, capacity)
    send_pos = jnp.einsum("tkr,t->r", table_a, position).reshape(experts, capacity)
    got_rows, got_pos = (
        lax.all_to_all(send_rows, "expert", split_axis=0, concat_axis=0, tiled=True),
        lax.all_to_all(send_pos, "expert", split_axis=0, concat_axis=0, tiled=True),
    )
    routed_one = got_rows.reshape(row_count, width)
    slot_pos = got_pos.reshape(row_count)
    query = weight_fold(routed_one, w_query[0]).astype(jnp.bfloat16)
    query_heads = query.reshape(row_count, HEADS, HEAD_DIM)

    def stat_step(carry_in, key_heads, value_heads, key_pos):
        highest, running = carry_in
        scores, allowed = masked_scores(query_heads, key_heads, slot_pos, key_pos)
        new_high = jnp.maximum(highest, jnp.max(jnp.where(allowed, scores, -1e30), axis=-1))
        running = running * jnp.exp(highest - new_high) + jnp.sum(
            jnp.where(allowed, jnp.exp(scores - new_high[:, :, None]), 0.0), axis=-1
        )
        return (new_high, running)

    highest, running = key_fold(
        kv_rows,
        stat_step,
        (
            jnp.full((HEADS, row_count), -1e30, jnp.float32),
            jnp.zeros((HEADS, row_count), jnp.float32),
        ),
    )
    log_norm = highest + jnp.log(running)

    def value_step(carry_in, key_heads, value_heads, key_pos):
        scores, allowed = masked_scores(query_heads, key_heads, slot_pos, key_pos)
        probabilities = jnp.where(allowed, jnp.exp(scores - log_norm[:, :, None]), 0.0).astype(
            jnp.bfloat16
        )
        return carry_in + jnp.einsum(
            "hrk,khd->rhd", probabilities, value_heads, preferred_element_type=jnp.float32
        )

    attended = key_fold(kv_rows, value_step, jnp.zeros((row_count, HEADS, HEAD_DIM), jnp.float32))
    attended = attended.reshape(row_count, QD).astype(jnp.bfloat16)
    branch_rows = weight_fold(attended, w_out[0]).astype(jnp.bfloat16)
    branch_back = to_home(branch_rows.reshape(experts, capacity, width))
    branch_pairs = collect_pairs(low_table_a, branch_back)
    residual_one = x_float + jnp.sum(shares_a[:, :, None] * branch_pairs, axis=1)
    scale_two = rms_scale(residual_one)
    normed_two = (residual_one * scale_two * norm2_gain).astype(jnp.bfloat16)
    shares_f, picked_f = pair_gates(
        jnp.dot(normed_two, ffn_router, preferred_element_type=jnp.float32),
        ffn_routes[0],
        live,
        experts,
    )
    table_f = route_table(ffn_routes[0], live_int, experts, capacity)
    low_table_f = table_f.astype(jnp.bfloat16)
    routed_two = to_owner(dispatch(low_table_f, normed_two, experts, capacity)).reshape(
        row_count, width
    )
    both = unit_forward(routed_two, w_in[0])
    hidden = (jax.nn.silu(both[:, :FF]) * both[:, FF:]).astype(jnp.bfloat16)
    down_rows = weight_fold(hidden, w_down[0]).astype(jnp.bfloat16)
    down_back = to_home(down_rows.reshape(experts, capacity, width))
    down_pairs = collect_pairs(low_table_f, down_back)
    mixed = jnp.sum(shares_f[:, :, None] * down_pairs, axis=1)
    layer_output = (live[:, None] * (residual_one + mixed)).astype(jnp.bfloat16)
    grad_out = output_grad[0].astype(jnp.float32) * live[:, None]
    pair_grad_f = jnp.sum(grad_out[:, None, :] * down_pairs, axis=-1)
    d_down = to_owner(spread_back(table_f, shares_f, grad_out, experts, capacity)).reshape(
        row_count, width
    )
    d_hidden = weight_back(d_down, w_down[0])
    gate_part = both[:, :FF]
    up_part = both[:, FF:]
    sigmoid_gate = jax.nn.sigmoid(gate_part)
    d_gate = d_hidden * up_part * sigmoid_gate * (1.0 + gate_part * (1.0 - sigmoid_gate))
    d_up = d_hidden * gate_part * sigmoid_gate
    d_gate_up = jnp.concatenate([d_gate, d_up], axis=1).astype(jnp.bfloat16)
    d_routed_two = unit_backward(d_gate_up, w_in[0]).astype(jnp.bfloat16)
    grad_w_in = unit_grad(d_gate_up, routed_two)
    grad_w_down = weight_grad(hidden, d_down)
    d_copy_two = to_home(d_routed_two.reshape(experts, capacity, width))
    dlog_f = logit_grad(shares_f, picked_f, pair_grad_f)
    d_normed_two = collect_sum(low_table_f, d_copy_two) + jnp.dot(
        dlog_f, ffn_router.astype(jnp.float32).T, precision=PRECISE
    )
    local_ffn_router = jnp.dot(normed_two.astype(jnp.float32).T, dlog_f, precision=PRECISE)
    d_mid, local_gain_two = norm_back(residual_one, scale_two, norm2_gain, d_normed_two)
    d_residual = grad_out + d_mid
    pair_grad_a = jnp.sum(d_residual[:, None, :] * branch_pairs, axis=-1)
    d_branch = to_owner(spread_back(table_a, shares_a, d_residual, experts, capacity)).reshape(
        row_count, width
    )
    d_attended = weight_back(d_branch, w_out[0]).astype(jnp.bfloat16)
    grad_w_out = weight_grad(attended, d_branch)
    delta_rows = jnp.sum(
        (d_attended.astype(jnp.float32) * attended.astype(jnp.float32)).reshape(
            row_count, HEADS, HEAD_DIM
        ),
        axis=-1,
    )
    delta_sum = delta_rows.T
    d_attended_heads = d_attended.reshape(row_count, HEADS, HEAD_DIM)

    def query_grad_step(carry_in, key_heads, value_heads, key_pos):
        scores, allowed = masked_scores(query_heads, key_heads, slot_pos, key_pos)
        probabilities = jnp.where(allowed, jnp.exp(scores - log_norm[:, :, None]), 0.0)
        d_prob = jnp.einsum(
            "rhd,khd->hrk", d_attended_heads, value_heads, preferred_element_type=jnp.float32
        )
        d_scores = (probabilities * (d_prob - delta_sum[:, :, None])).astype(jnp.bfloat16)
        return carry_in + jnp.einsum(
            "hrk,khd->rhd", d_scores, key_heads, preferred_element_type=jnp.float32
        )

    d_query_sum = key_fold(
        kv_rows, query_grad_step, jnp.zeros((row_count, HEADS, HEAD_DIM), jnp.float32)
    )
    d_query = (d_query_sum * HEAD_DIM ** (-0.5)).reshape(row_count, QD).astype(jnp.bfloat16)
    d_routed_one = weight_back(d_query, w_query[0]).astype(jnp.bfloat16)
    grad_w_query = weight_grad(routed_one, d_query)
    d_copy_one = to_home(d_routed_one.reshape(experts, capacity, width))
    own_keys = kv_rows[:, :QD].reshape(tokens, HEADS, HEAD_DIM)
    own_values = kv_rows[:, QD:].reshape(tokens, HEADS, HEAD_DIM)
    zeros_heads = jnp.zeros((tokens, HEADS, HEAD_DIM), jnp.float32)
    carried = (zeros_heads, zeros_heads)
    shard_piece = (
        lax.all_gather(query, ("expert", "context"), axis=0, tiled=True),
        lax.all_gather(d_attended, ("expert", "context"), axis=0, tiled=True),
        lax.all_gather(
            log_norm.T.astype(jnp.bfloat16), ("expert", "context"), axis=0, tiled=True
        ).astype(jnp.float32),
        lax.all_gather(
            delta_rows.astype(jnp.bfloat16), ("expert", "context"), axis=0, tiled=True
        ).astype(jnp.float32),
        lax.all_gather(slot_pos, ("expert", "context"), axis=0, tiled=True),
    )
    piece_len = shard_piece[0].shape[0]
    block_len = math.gcd(piece_len, row_count)

    def body_one_block(carry_in, element):
        query_part, grad_part, norm_part, delta_part, pos_part = element
        query_low = query_part.reshape(block_len, HEADS, HEAD_DIM)
        grad_low = grad_part.reshape(block_len, HEADS, HEAD_DIM)
        scores, allowed = masked_scores(query_low, own_keys, pos_part, position)
        probabilities = jnp.where(allowed, jnp.exp(scores - norm_part.T[:, :, None]), 0.0)
        d_prob = jnp.einsum(
            "rhd,khd->hrk", grad_low, own_values, preferred_element_type=jnp.float32
        )
        d_scores = (probabilities * (d_prob - delta_part.T[:, :, None])).astype(jnp.bfloat16)
        d_keys, d_values = carry_in
        d_keys = d_keys + jnp.einsum(
            "hrk,rhd->khd", d_scores, query_low, preferred_element_type=jnp.float32
        )
        d_values = d_values + jnp.einsum(
            "hrk,rhd->khd",
            probabilities.astype(jnp.bfloat16),
            grad_low,
            preferred_element_type=jnp.float32,
        )
        return ((d_keys, d_values), None)

    shaped = tuple(
        (
            member.reshape((piece_len // block_len, block_len) + member.shape[1:])
            for member in shard_piece
        )
    )
    carried, _ = lax.scan(body_one_block, carried, shaped)
    d_keys, d_values = carried
    d_kv = jnp.concatenate(
        [d_keys.reshape(tokens, QD) * HEAD_DIM ** (-0.5), d_values.reshape(tokens, QD)], axis=1
    ).astype(jnp.bfloat16)
    grad_w_kv = lax.psum(weight_grad(normed_one, d_kv).astype(jnp.bfloat16), "expert").astype(
        jnp.float32
    )
    dlog_a = logit_grad(shares_a, picked_a, pair_grad_a)
    d_normed_one = (
        collect_sum(low_table_a, d_copy_one)
        + weight_back(d_kv, w_kv)
        + jnp.dot(dlog_a, attn_router.astype(jnp.float32).T, precision=PRECISE)
    )
    local_attn_router = jnp.dot(normed_one.astype(jnp.float32).T, dlog_a, precision=PRECISE)
    d_first, local_gain_one = norm_back(x_float, scale_one, norm1_gain, d_normed_one)
    input_grad = d_residual + d_first
    gain_one_sum, gain_two_sum, router_a_sum, router_f_sum = lax.psum(
        (local_gain_one, local_gain_two, local_attn_router, local_ffn_router),
        ("expert", "context", "dp"),
    )
    return (
        layer_output[None],
        input_grad[None],
        gain_one_sum,
        gain_two_sum,
        router_a_sum,
        router_f_sum,
        grad_w_kv,
        grad_w_query[None],
        grad_w_out[None],
        grad_w_in[None],
        grad_w_down[None],
    )


MESH = pl.DeviceIdType.MESH
EVERY = ("dp", "expert", "context")
SHARE = ("context", "dp")

class Place:
    def __init__(self):
        self.e = lax.axis_index("expert"); self.x = lax.axis_index("context"); self.z = lax.axis_index("dp")
        self.own = (self.e, self.x)
        self.c = lax.rem(self.e, 2)
        self.sib = (self.e + 1 - 2 * self.c, self.x)
        self.cols = self.columns(self.e, self.x, self.c)
        self.sib_cols = self.columns(self.sib[0], self.x, 1 - self.c)
    def columns(self, e, x, c):
        first = (lax.rem(e + 2 * c, 4), lax.rem(x + 1 - c, 2))
        second = (lax.rem(e + 2 * (1 - c), 4), lax.rem(x + c, 2))
        diag = (lax.rem(e + 2, 4), 1 - x)
        return ((e, x), first, second, diag)
    def dev(self, col, z=None):
        return (col[0], col[1], self.z if z is None else z)
    def block(self, col, z):
        return z * 8 + col[0] * 2 + col[1]

def greet(pc, sides):
    barrier = pltpu.get_barrier_semaphore()
    for col in (pc.sib, pc.cols[1], pc.cols[2]):
        pl.semaphore_signal(barrier, inc=1, device_id=pc.dev(col), device_id_type=MESH)
    @pl.when(pc.z > 0)
    def _():
        pl.semaphore_signal(barrier, inc=1, device_id=pc.dev(pc.own, pc.z - 1), device_id_type=MESH)
    @pl.when(pc.z < sides - 1)
    def _():
        pl.semaphore_signal(barrier, inc=1, device_id=pc.dev(pc.own, pc.z + 1), device_id_type=MESH)
    pl.semaphore_wait(barrier, 3 + lax.div(pc.z + sides - 1, sides) + lax.div(2 * sides - 2 - pc.z, sides))


def gather_kernel(x_ref, out_ref, loc, zs, zr, fs, fr, ss, sr, bs, br):
    pc = Place()
    z = pc.z
    mine = pltpu.make_async_copy(x_ref, out_ref.at[pc.block(pc.own, z)], loc)
    mine.start()
    greet(pc, 4)
    def rc(src, blk, s, r, dev):
        return pltpu.make_async_remote_copy(src_ref=src, dst_ref=out_ref.at[blk], send_sem=s, recv_sem=r, device_id=dev, device_id_type=MESH)
    def hop(col, d, kind):
        zz = z + d
        blk = pc.block(pc.cols[col], zz)
        src = x_ref if (col == 0 and d == 0) else out_ref.at[blk]
        i = d + 3
        if kind == "f":
            return rc(src, blk, fs.at[i], fr.at[i], pc.dev(pc.cols[1]))
        if kind == "s":
            return rc(src, blk, ss.at[col, i], sr.at[col, i], pc.dev(pc.cols[2]))
        return rc(src, blk, bs.at[col, i], br.at[col, i], pc.dev(pc.sib))
    def zhop(d, up):
        zz = z + d
        blk = pc.block(pc.own, zz)
        src = x_ref if d == 0 else out_ref.at[blk]
        i = 0 if up else 1
        return rc(src, blk, zs.at[i, abs(d)], zr.at[i, abs(d)], pc.dev(pc.own, z + 1 if up else z - 1))
    def ok(d):
        return (z + d >= 0) & (z + d <= 3)
    def when(cond, f):
        if cond is True:
            f()
        else:
            pl.when(cond)(f)
    def start_z(d):
        if d <= 0:
            pl.when(ok(d) & (z < 3))(lambda: zhop(d, True).start())
        if d >= 0:
            pl.when(ok(d) & (z > 0))(lambda: zhop(d, False).start())
    def own_line(d):
        def go():
            if d < 0:
                rc(out_ref.at[0], pc.block(pc.own, z + d), zs.at[0, -d - 1], zr.at[0, -d - 1], pc.dev(pc.own)).wait_recv()
            if d > 0:
                rc(out_ref.at[0], pc.block(pc.own, z + d), zs.at[1, d - 1], zr.at[1, d - 1], pc.dev(pc.own)).wait_recv()
            if d <= 0:
                pl.when(z < 3)(lambda: zhop(d, True).start())
            if d >= 0:
                pl.when(z > 0)(lambda: zhop(d, False).start())
            hop(0, d, "f").start()
            hop(0, d, "s").start()
            hop(0, d, "b").start()
        when(True if d == 0 else ok(d), go)
    def first_col(d):
        def go():
            blk = pc.block(pc.cols[1], z + d)
            rc(out_ref.at[0], blk, fs.at[d + 3], fr.at[d + 3], pc.dev(pc.own)).wait_recv()
            hop(1, d, "s").start()
            hop(1, d, "b").start()
        when(True if d == 0 else ok(d), go)
    def last_cols(d):
        def go():
            for col, j in ((2, 0), (3, 1)):
                blk = pc.block(pc.cols[col], z + d)
                rc(out_ref.at[0], blk, ss.at[j, d + 3], sr.at[j, d + 3], pc.dev(pc.own)).wait_recv()
                hop(col, d, "b").start()
        when(True if d == 0 else ok(d), go)
    own_line(0)
    for s in (1, 2, 3):
        own_line(-s); own_line(s)
        if s == 1:
            first_col(0)
        else:
            first_col(-(s - 1)); first_col(s - 1)
    first_col(-3); first_col(3)
    for d in (0, -1, 1, -2, 2, -3, 3):
        last_cols(d)
    for d in (0, -1, 1, -2, 2, -3, 3):
        def go():
            for j in range(4):
                blk = pc.block(pc.sib_cols[j], z + d)
                rc(out_ref.at[0], blk, bs.at[j, d + 3], br.at[j, d + 3], pc.dev(pc.own)).wait_recv()
            hop(0, d, "f").wait_send()
            for col in (0, 1):
                hop(col, d, "s").wait_send()
            for col in range(4):
                hop(col, d, "b").wait_send()
            if d <= 0:
                pl.when(z < 3)(lambda: zhop(d, True).wait_send())
            if d >= 0:
                pl.when(z > 0)(lambda: zhop(d, False).wait_send())
        when(True if d == 0 else ok(d), go)
    mine.wait()

def gather_all(x, cid):
    rows, width = x.shape
    D = pltpu.SemaphoreType.DMA
    out = pl.pallas_call(
        gather_kernel,
        out_shape=jax.ShapeDtypeStruct((32, rows, width), x.dtype),
        in_specs=[pl.BlockSpec(memory_space=pltpu.VMEM)],
        out_specs=pl.BlockSpec(memory_space=pl.ANY),
        scratch_shapes=[D, D((2, 4)), D((2, 4)), D((7,)), D((7,)), D((2, 7)), D((2, 7)), D((4, 7)), D((4, 7))],
        compiler_params=pltpu.CompilerParams(collective_id=cid, has_side_effects=True),
        name="gather_all",
    )(x)
    return out.reshape(32 * rows, width)

def scatter_kernel(p_ref, out_ref, acc, sib, sec, fst, zin, ld, bs, br, ss, sr, fs, fr, zs, zr):
    pc = Place()
    z = pc.z
    rows = p_ref.shape[1]
    inner = lax.rem(lax.div(z + 1, 2), 2)
    low = 1 - lax.div(z, 2)
    gray = (0, 1, 3, 2)
    def group(k):
        v = (1 - inner) * k + inner * gray[k]
        return low * (3 - v) + (1 - low) * v
    def rc(src, dst, s, r, dev):
        return pltpu.make_async_remote_copy(src_ref=src, dst_ref=dst, send_sem=s, recv_sem=r, device_id=dev, device_id_type=MESH)
    def load(k, col):
        return pltpu.make_async_copy(p_ref.at[pc.block(pc.cols[col], group(k))], acc.at[k, col], ld.at[k, col])
    def to_sib(k, col):
        return rc(p_ref.at[pc.block(pc.sib_cols[col], group(k))], sib.at[k, col], bs.at[k, col], br.at[k, col], pc.dev(pc.sib))
    def to_second(k, j):
        return rc(acc.at[k, 2 + j], sec.at[k, j], ss.at[k, j], sr.at[k, j], pc.dev(pc.cols[2]))
    def to_first(k):
        return rc(acc.at[k, 1], fst.at[k], fs.at[k], fr.at[k], pc.dev(pc.cols[1]))
    def to_z(k, up):
        g = group(k)
        i = 0 if up else 1
        return rc(acc.at[k, 0], zin.at[i, g], zs.at[i, k], zr.at[i, g], pc.dev(pc.own, z + 1 if up else z - 1))
    def from_z(g, i):
        return rc(acc.at[0, 0], zin.at[i, g], zs.at[i, 0], zr.at[i, g], pc.dev(pc.own))
    step = 16
    def add(k, col, other):
        def body(i, carry):
            r = pl.ds(pl.multiple_of(i * step, step), step)
            acc[k, col, r, :] = (acc[k, col, r, :].astype(jnp.float32) + other[r, :].astype(jnp.float32)).astype(acc.dtype)
            return carry
        lax.fori_loop(0, rows // step, body, 0)
    for k in range(4):
        for col in (2, 3, 1, 0):
            load(k, col).start()
    greet(pc, 4)
    for k in range(4):
        for col in (2, 3, 1, 0):
            to_sib(k, col).start()
    def join(k, col):
        load(k, col).wait()
        to_sib(k, col).wait_recv()
        add(k, col, sib.at[k, col])
    def stage_a(k):
        for j in (0, 1):
            join(k, 2 + j)
            to_second(k, j).start()
    def stage_b(k):
        join(k, 1)
        to_second(k, 1).wait_recv()
        add(k, 1, sec.at[k, 1])
        to_first(k).start()
        join(k, 0)
    def stage_c(k):
        to_second(k, 0).wait_recv()
        add(k, 0, sec.at[k, 0])
        to_first(k).wait_recv()
        add(k, 0, fst.at[k])
        g = group(k)
        if k < 3:
            @pl.when(g > z)
            def _():
                @pl.when(z > 0)
                def _():
                    from_z(g, 0).wait_recv()
                    add(k, 0, zin.at[0, g])
                to_z(k, True).start()
            @pl.when(g < z)
            def _():
                @pl.when(z < 3)
                def _():
                    from_z(g, 1).wait_recv()
                    add(k, 0, zin.at[1, g])
                to_z(k, False).start()
        else:
            @pl.when(z > 0)
            def _():
                from_z(z, 0).wait_recv()
                add(k, 0, zin.at[0, z])
            @pl.when(z < 3)
            def _():
                from_z(z, 1).wait_recv()
                add(k, 0, zin.at[1, z])
    stage_a(0); stage_a(1); stage_b(0); stage_a(2); stage_b(1); stage_c(0)
    stage_a(3); stage_b(2); stage_c(1); stage_b(3); stage_c(2); stage_c(3)
    out_ref[...] = acc[3, 0]
    for k in range(4):
        for col in range(4):
            to_sib(k, col).wait_send()
        for j in (0, 1):
            to_second(k, j).wait_send()
        to_first(k).wait_send()
        if k < 3:
            pl.when(group(k) > z)(lambda: to_z(k, True).wait_send())
            pl.when(group(k) < z)(lambda: to_z(k, False).wait_send())

def scatter_all(p, cid):
    total, width = p.shape
    rows = total // 32
    D = pltpu.SemaphoreType.DMA
    V = lambda *s: pltpu.VMEM(s + (rows, width), p.dtype)
    return pl.pallas_call(
        scatter_kernel,
        out_shape=jax.ShapeDtypeStruct((rows, width), p.dtype),
        in_specs=[pl.BlockSpec(memory_space=pl.ANY)],
        out_specs=pl.BlockSpec(memory_space=pltpu.VMEM),
        scratch_shapes=[V(4, 4), V(4, 4), V(4, 2), V(4), V(2, 4), D((4, 4)), D((4, 4)), D((4, 4)), D((4, 2)), D((4, 2)), D((4,)), D((4,)), D((2, 4)), D((2, 4))],
        compiler_params=pltpu.CompilerParams(collective_id=cid, has_side_effects=True, vmem_limit_bytes=48 << 20),
        name="scatter_all",
    )(p.reshape(32, rows, width))


def attend_kernel(qkv_ref, att_ref, lse_ref):
    length = qkv_ref.shape[0]
    tile = 256
    heads = att_ref.shape[1] // HEAD_DIM
    for head in range(heads):
        at = lambda part: pl.ds((part * heads + head) * HEAD_DIM, HEAD_DIM)
        for first in range(0, length, tile):
            last = first + tile
            q = qkv_ref[pl.ds(first, tile), at(0)]
            k = qkv_ref[pl.ds(0, last), at(1)]
            v = qkv_ref[pl.ds(0, last), at(2)]
            scores = lax.dot_general(
                k, q, (((1,), (1,)), ((), ())), preferred_element_type=jnp.float32
            ) * HEAD_DIM ** (-0.5)
            key_pos = lax.broadcasted_iota(jnp.int32, scores.shape, 0)
            query_pos = first + lax.broadcasted_iota(jnp.int32, scores.shape, 1)
            scores = jnp.where(key_pos <= query_pos, scores, -1e30)
            highest = jnp.max(scores, axis=0, keepdims=True)
            exponent = jnp.exp(scores - highest)
            total = jnp.sum(exponent, axis=0, keepdims=True)
            mixed = lax.dot_general(
                v,
                exponent.astype(jnp.bfloat16),
                (((0,), (0,)), ((), ())),
                preferred_element_type=jnp.float32,
            )
            mixed = mixed * (1.0 / total)
            att_ref[pl.ds(first, tile), pl.ds(head * HEAD_DIM, HEAD_DIM)] = mixed.T.astype(
                jnp.bfloat16
            )
            lse_ref[0, pl.ds(head, 1), pl.ds(first, tile)] = highest + jnp.log(total)


def attend(qkv, slots):
    rows, width = qkv.shape
    length = rows // slots
    out = width // 3
    return pl.pallas_call(
        attend_kernel,
        grid=(slots,),
        out_shape=(
            jax.ShapeDtypeStruct((rows, out), jnp.bfloat16),
            jax.ShapeDtypeStruct((slots, out // HEAD_DIM, length), jnp.float32),
        ),
        in_specs=[pl.BlockSpec((length, width), lambda s: (s, 0))],
        out_specs=(
            pl.BlockSpec((length, out), lambda s: (s, 0)),
            pl.BlockSpec((1, out // HEAD_DIM, length), lambda s: (s, 0, 0)),
        ),
        compiler_params=pltpu.CompilerParams(vmem_limit_bytes=48 << 20),
        name="attend",
    )(qkv)


def attend_back_kernel(qkv_ref, du_ref, lse_ref, gate_ref, dqkv_ref, dgate_ref, dk_acc, dv_acc):
    length = qkv_ref.shape[0]
    tile = 256
    heads = du_ref.shape[1] // HEAD_DIM
    scale = HEAD_DIM ** (-0.5)
    for head in range(heads):
        at = lambda part: pl.ds((part * heads + head) * HEAD_DIM, HEAD_DIM)
        dk_acc[...] = jnp.zeros_like(dk_acc)
        dv_acc[...] = jnp.zeros_like(dv_acc)
        for first in range(0, length, tile):
            last = first + tile
            q = qkv_ref[pl.ds(first, tile), at(0)]
            k = qkv_ref[pl.ds(0, last), at(1)]
            v = qkv_ref[pl.ds(0, last), at(2)]
            du = du_ref[pl.ds(first, tile), pl.ds(head * HEAD_DIM, HEAD_DIM)]
            gate = gate_ref[0, :, pl.ds(first, tile)]
            lse = lse_ref[0, pl.ds(head, 1), pl.ds(first, tile)]
            scores = (
                lax.dot_general(k, q, (((1,), (1,)), ((), ())), preferred_element_type=jnp.float32)
                * scale
            )
            key_pos = lax.broadcasted_iota(jnp.int32, scores.shape, 0)
            query_pos = first + lax.broadcasted_iota(jnp.int32, scores.shape, 1)
            probs = jnp.where(key_pos <= query_pos, jnp.exp(scores - lse), 0.0)
            d_prob = lax.dot_general(
                v, du, (((1,), (1,)), ((), ())), preferred_element_type=jnp.float32
            )
            along = jnp.sum(probs * d_prob, axis=0, keepdims=True)
            dgate_ref[0, pl.ds(head, 1), pl.ds(first, tile)] = along
            shared = probs * gate
            d_scores = (shared * (d_prob - along)).astype(jnp.bfloat16)
            dq = lax.dot_general(
                d_scores, k, (((0,), (0,)), ((), ())), preferred_element_type=jnp.float32
            )
            dqkv_ref[pl.ds(first, tile), at(0)] = (dq * scale).astype(jnp.bfloat16)
            dk_acc[pl.ds(0, last), :] += jnp.dot(d_scores, q, preferred_element_type=jnp.float32)
            dv_acc[pl.ds(0, last), :] += jnp.dot(
                shared.astype(jnp.bfloat16), du, preferred_element_type=jnp.float32
            )
        dqkv_ref[:, at(1)] = (dk_acc[...] * scale).astype(jnp.bfloat16)
        dqkv_ref[:, at(2)] = dv_acc[...].astype(jnp.bfloat16)


def attend_back(qkv, du, lse, gate, slots):
    rows, width = qkv.shape
    length = rows // slots
    out = width // 3
    heads = out // HEAD_DIM
    return pl.pallas_call(
        attend_back_kernel,
        grid=(slots,),
        out_shape=(
            jax.ShapeDtypeStruct((rows, width), jnp.bfloat16),
            jax.ShapeDtypeStruct((slots, heads, length), jnp.float32),
        ),
        in_specs=[
            pl.BlockSpec((length, width), lambda s: (s, 0)),
            pl.BlockSpec((length, out), lambda s: (s, 0)),
            pl.BlockSpec((1, heads, length), lambda s: (s, 0, 0)),
            pl.BlockSpec((1, 1, length), lambda s: (s, 0, 0)),
        ],
        out_specs=(
            pl.BlockSpec((length, width), lambda s: (s, 0)),
            pl.BlockSpec((1, heads, length), lambda s: (s, 0, 0)),
        ),
        scratch_shapes=[
            pltpu.VMEM((length, HEAD_DIM), jnp.float32),
            pltpu.VMEM((length, HEAD_DIM), jnp.float32),
        ],
        compiler_params=pltpu.CompilerParams(vmem_limit_bytes=48 << 20),
        name="attend_back",
    )(qkv, du, lse, gate)


def spread(per_token):
    columns = per_token.T.reshape(1, -1)
    whole = lax.all_gather(columns, EVERY, axis=0, tiled=True)
    return whole.reshape(whole.shape[0], per_token.shape[1], per_token.shape[0])


def home_sums(per_expert, experts):
    devices, tokens = per_expert.shape
    mine = (jnp.arange(experts) == lax.axis_index("expert")).astype(jnp.float32)
    columns = (per_expert[:, None, :] * mine[None, :, None]).reshape(devices, experts * tokens)
    return lax.psum_scatter(columns, EVERY, scatter_dimension=0, tiled=True).reshape(experts, tokens).T


def placed_weights(
    layer_input,
    output_grad,
    lengths,
    attn_routes,
    ffn_routes,
    norm1_gain,
    norm2_gain,
    attn_router,
    ffn_router,
    w_kv,
    w_query,
    w_out,
    w_in,
    w_down,
):
    f32, low = jnp.float32, jnp.bfloat16
    tokens, width = layer_input.shape[1:]
    experts = lax.axis_size("expert")
    contexts = lax.axis_size("context")
    slots = lax.axis_size("dp")
    shares = contexts * slots
    devices = experts * shares
    own_expert = lax.axis_index("expert")
    capacity = tokens * TOP // experts + tokens // 32
    room = -(-capacity // 8) * 8

    position = lax.axis_index(("expert", "context")) * tokens + jnp.arange(tokens, dtype=jnp.int32)
    live = (position < lengths[0]).astype(f32)
    x_float = layer_input[0].astype(f32)
    scale_one = rms_scale(x_float)
    normed_one = (x_float * scale_one * norm1_gain).astype(low)
    grad_out = output_grad[0].astype(f32) * live[:, None]

    kv_parts = w_kv.reshape(-1, 2, shares, QD // shares).transpose(0, 2, 1, 3)
    qkv_parts = jnp.concatenate(
        [w_query[0].reshape(-1, shares, QD // shares), kv_parts.reshape(kv_parts.shape[0], shares, -1)],
        axis=2,
    )
    piece = qkv_parts.shape[2]
    w_qkv = lax.all_to_all(
        qkv_parts.reshape(-1, shares * piece), SHARE, split_axis=1, concat_axis=0, tiled=True
    )
    w_pair = lax.all_to_all(w_in[0], "context", split_axis=0, concat_axis=0, tiled=True)
    moves = [(s, (s % contexts) * slots + s // contexts) for s in range(shares)]
    w_unit = lax.ppermute(w_down[0], SHARE, moves)
    units = w_unit.shape[0]

    all_one = gather_all(normed_one, 0)
    shares_a, picked_a = pair_gates(
        jnp.dot(normed_one, attn_router, preferred_element_type=f32), attn_routes[0], live, experts
    )
    gates_a = jnp.sum(shares_a[:, :, None] * picked_a, axis=1)
    named_f = jnp.sum(
        (ffn_routes[0][:, :, None] == jnp.arange(experts, dtype=jnp.int32)).astype(f32), axis=1
    )
    aux = lax.dynamic_index_in_dim(
        spread(jnp.concatenate([gates_a, named_f * live[:, None]], axis=1)).reshape(
            devices, 2, experts, tokens
        ),
        own_expert,
        axis=2,
        keepdims=False,
    )
    gate_a, named = aux[:, 0], aux[:, 1]
    all_grad = lax.all_gather(grad_out.astype(low), EVERY, axis=0, tiled=True)
    qkv = jnp.dot(all_one, w_qkv, preferred_element_type=f32).astype(low)
    attended, lse = attend(qkv, slots)
    gated = (attended.astype(f32) * gate_a.reshape(-1, 1)).astype(low)
    h1_part = jnp.dot(gated, w_out[0], preferred_element_type=f32).astype(low)
    residual_one = x_float + scatter_all(h1_part, 1).astype(f32)

    scale_two = rms_scale(residual_one)
    normed_two = (residual_one * scale_two * norm2_gain).astype(low)
    all_two = gather_all(normed_two, 2)
    shares_f, picked_f = pair_gates(
        jnp.dot(normed_two, ffn_router, preferred_element_type=f32), ffn_routes[0], live, experts
    )
    gates_f = jnp.sum(shares_f[:, :, None] * picked_f, axis=1)
    gate_f = lax.dynamic_index_in_dim(spread(gates_f), own_expert, axis=1, keepdims=False)
    earlier = (jnp.arange(tokens)[:, None] < jnp.arange(tokens)[None, :]).astype(f32)
    rank = jnp.dot(named, earlier, preferred_element_type=f32)
    table = jnp.where(
        rank[:, None, :] == jnp.arange(room, dtype=f32)[None, :, None], named[:, None, :], 0.0
    )
    low_table = table.astype(low)

    def pick(whole):
        rows = jnp.einsum(
            "bst,btd->bsd",
            low_table,
            whole.reshape(devices, tokens, width),
            preferred_element_type=f32,
        )
        return rows.astype(low).reshape(devices * room, width)

    def put(rows):
        whole = jnp.einsum(
            "bst,bsd->btd", low_table, rows.reshape(devices, room, width), preferred_element_type=f32
        )
        return whole.astype(low).reshape(devices * tokens, width)

    row_gate = jnp.sum(table * gate_f[:, None, :], axis=2).reshape(-1, 1)
    routed = pick(all_two)
    both = lax.dot_general(routed, w_pair, (((1,), (1,)), ((), ())), preferred_element_type=f32)
    gate_part, up_part = both[:, :units], both[:, units:]
    sigmoid_gate = jax.nn.sigmoid(gate_part)
    hidden_f = gate_part * sigmoid_gate * up_part
    hidden = hidden_f.astype(low)
    down = (jnp.dot(hidden, w_unit, preferred_element_type=f32) * row_gate).astype(low)
    mixed = scatter_all(put(down), 3).astype(f32)
    layer_output = (live[:, None] * (residual_one + mixed)).astype(low)

    d_rows = pick(all_grad)
    d_plain = lax.dot_general(d_rows, w_unit, (((1,), (1,)), ((), ())), preferred_element_type=f32)
    row_sums = jnp.sum(d_plain * hidden.astype(f32), axis=1).reshape(devices, room)
    dgate_f = home_sums(jnp.sum(table * row_sums[:, :, None], axis=1), experts)
    d_hidden = d_plain * row_gate
    d_gate = d_hidden * up_part * sigmoid_gate * (1.0 + gate_part * (1.0 - sigmoid_gate))
    d_up = d_hidden * gate_part * sigmoid_gate
    d_both = jnp.concatenate([d_gate, d_up], axis=1).astype(low)
    d_two_part = put(jnp.dot(d_both, w_pair, preferred_element_type=f32).astype(low))
    grad_unit = lax.dot_general(
        (hidden.astype(f32) * row_gate).astype(low),
        d_rows,
        (((0,), (0,)), ((), ())),
        preferred_element_type=f32,
    )
    grad_pair = lax.dot_general(
        d_both, routed, (((0,), (0,)), ((), ())), preferred_element_type=f32
    )
    grad_w_in = lax.all_to_all(
        grad_pair.astype(low), "context", split_axis=0, concat_axis=0, tiled=True
    ).astype(f32)
    grad_w_down = lax.ppermute(grad_unit.astype(low), SHARE, [(b, a) for a, b in moves]).astype(f32)
    dlog_f = gates_f * (dgate_f - jnp.sum(gates_f * dgate_f, axis=1, keepdims=True))
    d_normed_two = scatter_all(d_two_part, 4).astype(f32) + jnp.dot(
        dlog_f, ffn_router.astype(f32).T, precision=PRECISE
    )
    local_ffn_router = jnp.dot(normed_two.astype(f32).T, dlog_f, precision=PRECISE)
    d_mid, local_gain_two = norm_back(residual_one, scale_two, norm2_gain, d_normed_two)
    d_residual = grad_out + d_mid

    all_mid = gather_all(d_residual.astype(low), 5)
    d_att = lax.dot_general(
        all_mid, w_out[0], (((1,), (1,)), ((), ())), preferred_element_type=f32
    ).astype(low)
    d_qkv, head_sums = attend_back(
        qkv, d_att, lse, gate_a.reshape(slots, 1, -1), slots
    )
    grad_w_out = lax.dot_general(
        gated, all_mid, (((0,), (0,)), ((), ())), preferred_element_type=f32
    )
    dgate_a = home_sums(jnp.sum(head_sums, axis=1).reshape(devices, tokens), experts)
    d_one_part = lax.dot_general(
        d_qkv, w_qkv, (((1,), (1,)), ((), ())), preferred_element_type=f32
    ).astype(low)
    grad_qkv = lax.dot_general(
        all_one, d_qkv, (((0,), (0,)), ((), ())), preferred_element_type=f32
    ).astype(low)
    grad_parts = lax.all_to_all(grad_qkv, SHARE, split_axis=0, concat_axis=1, tiled=True)
    grad_parts = grad_parts.reshape(-1, shares, piece)
    grad_w_query = grad_parts[:, :, : QD // shares].reshape(-1, QD).astype(f32)
    kv_grads = grad_parts[:, :, QD // shares :].reshape(-1, shares, 2, QD // shares)
    grad_w_kv = lax.psum(kv_grads.transpose(0, 2, 1, 3).reshape(-1, 2 * QD), "expert").astype(f32)
    dlog_a = gates_a * (dgate_a - jnp.sum(gates_a * dgate_a, axis=1, keepdims=True))
    d_normed_one = scatter_all(d_one_part, 6).astype(f32) + jnp.dot(
        dlog_a, attn_router.astype(f32).T, precision=PRECISE
    )
    local_attn_router = jnp.dot(normed_one.astype(f32).T, dlog_a, precision=PRECISE)
    d_first, local_gain_one = norm_back(x_float, scale_one, norm1_gain, d_normed_one)
    input_grad = d_residual + d_first
    gain_one_sum, gain_two_sum, router_a_sum, router_f_sum = lax.psum(
        (local_gain_one, local_gain_two, local_attn_router, local_ffn_router),
        ("expert", "context", "dp"),
    )
    return (
        layer_output[None],
        input_grad[None],
        gain_one_sum,
        gain_two_sum,
        router_a_sum,
        router_f_sum,
        grad_w_kv,
        grad_w_query[None],
        grad_w_out[None],
        grad_w_in[None],
        grad_w_down[None],
    )


def fits_in_place(mesh):
    sizes = (mesh.shape["expert"], mesh.shape["context"], mesh.shape["dp"])
    return sizes == (4, 2, 4)


def solution(mesh):
    placed = (
        P("dp", ("expert", "context"), None),
        P("dp", ("expert", "context"), None),
        P("dp"),
        P("dp", ("expert", "context"), None),
        P("dp", ("expert", "context"), None),
        P(),
        P(),
        P(),
        P(),
        P(("context", "dp"), None),
        P("expert", ("context", "dp"), None),
        P("expert", ("context", "dp"), None),
        P("expert", ("context", "dp"), None),
        P("expert", ("context", "dp"), None),
    )
    return jax.shard_map(
        placed_weights if fits_in_place(mesh) else gathered_weights,
        mesh=mesh,
        in_specs=placed,
        out_specs=(
            P("dp", ("expert", "context"), None),
            P("dp", ("expert", "context"), None),
            P(),
            P(),
            P(),
            P(),
            P(("context", "dp"), None),
            P("expert", ("context", "dp"), None),
            P("expert", ("context", "dp"), None),
            P("expert", ("context", "dp"), None),
            P("expert", ("context", "dp"), None),
        ),
        check_vma=False,
    )
```

```python
import functools
import math

import jax
import jax.numpy as jnp
from jax import lax
from jax.experimental import pallas as pl
from jax.experimental.pallas import tpu as pltpu
from jax.sharding import PartitionSpec as P

HEADS = 16
HEAD_DIM = 128
FF = 5632
TOP = 2
QD = 2048


EPSILON = 1e-06
PRECISE = lax.Precision.HIGHEST


def rms_scale(value):
    return lax.rsqrt(jnp.mean(value * value, axis=-1, keepdims=True) + EPSILON)


def norm_back(value, scale, gain, grad_normed):
    weighted = grad_normed * gain
    d_gain = jnp.sum(grad_normed * value * scale, axis=0)
    d_value = scale * weighted - value * scale**3 * jnp.mean(
        weighted * value, axis=-1, keepdims=True
    )
    return (d_value, d_gain)


def weight_fold(left_rows, weight):
    return jnp.dot(
        left_rows,
        lax.all_gather(weight, ("context", "dp"), axis=0, tiled=True),
        preferred_element_type=jnp.float32,
    )


def weight_back(gradient, weight):
    return lax.dot_general(
        gradient,
        lax.all_gather(weight, ("context", "dp"), axis=0, tiled=True),
        (((1,), (1,)), ((), ())),
        preferred_element_type=jnp.float32,
    )


def weight_grad(left_rows, gradient):
    return lax.psum_scatter(
        lax.dot_general(
            left_rows, gradient, (((0,), (0,)), ((), ())), preferred_element_type=jnp.float32
        ).astype(jnp.bfloat16),
        ("context", "dp"),
        scatter_dimension=0,
        tiled=True,
    ).astype(jnp.float32)


def unit_forward(left_rows, weight):
    return lax.dot_general(
        left_rows,
        lax.all_gather(weight, ("context", "dp"), axis=0, tiled=True),
        (((1,), (1,)), ((), ())),
        preferred_element_type=jnp.float32,
    )


def unit_backward(gradient, weight):
    return jnp.dot(
        gradient,
        lax.all_gather(weight, ("context", "dp"), axis=0, tiled=True),
        preferred_element_type=jnp.float32,
    )


def unit_grad(gradient, left_rows):
    return lax.psum_scatter(
        lax.dot_general(
            gradient, left_rows, (((0,), (0,)), ((), ())), preferred_element_type=jnp.float32
        ).astype(jnp.bfloat16),
        ("context", "dp"),
        scatter_dimension=0,
        tiled=True,
    ).astype(jnp.float32)


def to_owner(slot_rows):
    return lax.all_to_all(slot_rows, "expert", split_axis=0, concat_axis=0, tiled=True)


def to_home(slot_rows):
    return lax.all_to_all(slot_rows, "expert", split_axis=0, concat_axis=0, tiled=True)


def pair_gates(logits, routes, live, experts):
    picked = (routes[:, :, None] == jnp.arange(experts, dtype=jnp.int32)[None, None, :]).astype(
        jnp.float32
    )
    chosen = jnp.sum(picked * logits[:, None, :], axis=-1)
    highest = jnp.max(chosen, axis=-1, keepdims=True)
    exponent = jnp.exp(chosen - highest)
    return (exponent / jnp.sum(exponent, axis=-1, keepdims=True) * live[:, None], picked)


def logit_grad(shares, picked, pair_grad):
    mean_grad = jnp.sum(shares * pair_grad, axis=-1, keepdims=True)
    return jnp.sum((shares * (pair_grad - mean_grad))[:, :, None] * picked, axis=1)


def route_table(routes, live_int, experts, capacity):
    owners = (routes[:, :, None] == jnp.arange(experts, dtype=jnp.int32)[None, None, :]).astype(
        jnp.int32
    )
    owners = owners * live_int[:, None, None]
    used_slots = jnp.sum(owners, axis=1)
    before = jnp.cumsum(used_slots, axis=0) - used_slots
    slot_rank = jnp.sum(before[:, None, :] * owners, axis=-1)
    target = routes * capacity + slot_rank
    slot_hits = (
        target[:, :, None] == jnp.arange(experts * capacity, dtype=jnp.int32)[None, None, :]
    ).astype(jnp.int32)
    return slot_hits * live_int[:, None, None]


def dispatch(table_low, token_rows, experts, capacity):
    sent = jnp.einsum("tkr,td->rd", table_low, token_rows, preferred_element_type=jnp.float32)
    return sent.astype(jnp.bfloat16).reshape(experts, capacity, token_rows.shape[1])


def collect_pairs(table_low, received):
    flat = received.reshape(-1, received.shape[-1])
    return jnp.einsum("tkr,rd->tkd", table_low, flat, preferred_element_type=jnp.float32)


def collect_sum(table_low, received):
    flat = received.reshape(-1, received.shape[-1])
    return jnp.einsum("tkr,rd->td", table_low, flat, preferred_element_type=jnp.float32)


def spread_back(table_int, shares, gradient, experts, capacity):
    weighted = shares[:, :, None] * gradient[:, None, :]
    sent = jnp.einsum("tkr,tkd->rd", table_int.astype(jnp.float32), weighted, precision=PRECISE)
    return sent.astype(jnp.bfloat16).reshape(experts, capacity, gradient.shape[1])


def masked_scores(query_heads, key_heads, query_pos, key_pos):
    scores = jnp.einsum(
        "rhd,khd->hrk", query_heads, key_heads, preferred_element_type=jnp.float32
    ) * HEAD_DIM ** (-0.5)
    return (scores, key_pos[None, None, :] <= query_pos[None, :, None])


def key_scan(shard_piece, block_step, carried):
    piece_len = shard_piece.shape[0]
    block_len = math.gcd(piece_len, 512)
    blocks = shard_piece.reshape(piece_len // block_len, block_len, shard_piece.shape[1])
    firsts = jnp.arange(piece_len // block_len, dtype=jnp.int32) * block_len

    def key_one_block(carry_in, element):
        block_rows, first_key = element
        key_heads = block_rows[:, :QD].reshape(block_len, HEADS, HEAD_DIM)
        value_heads = block_rows[:, QD:].reshape(block_len, HEADS, HEAD_DIM)
        key_pos = first_key + jnp.arange(block_len, dtype=jnp.int32)
        return (block_step(carry_in, key_heads, value_heads, key_pos), None)

    carried, _ = lax.scan(key_one_block, carried, (blocks, firsts))
    return carried


def key_fold(kv_rows, block_step, zeros_init):
    return key_scan(
        lax.all_gather(kv_rows, ("expert", "context"), axis=0, tiled=True), block_step, zeros_init
    )


def gathered_weights(
    layer_input,
    output_grad,
    lengths,
    attn_routes,
    ffn_routes,
    norm1_gain,
    norm2_gain,
    attn_router,
    ffn_router,
    w_kv,
    w_query,
    w_out,
    w_in,
    w_down,
):
    tokens = layer_input.shape[1]
    width = layer_input.shape[2]
    experts = lax.axis_size("expert")
    capacity = tokens * TOP // experts + tokens // 32
    row_count = experts * capacity
    position = lax.axis_index(("expert", "context")) * tokens + jnp.arange(tokens, dtype=jnp.int32)
    live_int = (position < lengths[0]).astype(jnp.int32)
    live = live_int.astype(jnp.float32)
    x_float = layer_input[0].astype(jnp.float32)
    scale_one = rms_scale(x_float)
    normed_one = (x_float * scale_one * norm1_gain).astype(jnp.bfloat16)
    kv_rows = weight_fold(normed_one, w_kv).astype(jnp.bfloat16)
    shares_a, picked_a = pair_gates(
        jnp.dot(normed_one, attn_router, preferred_element_type=jnp.float32),
        attn_routes[0],
        live,
        experts,
    )
    table_a = route_table(attn_routes[0], live_int, experts, capacity)
    low_table_a = table_a.astype(jnp.bfloat16)
    send_rows = dispatch(low_table_a, normed_one, experts, capacity)
    send_pos = jnp.einsum("tkr,t->r", table_a, position).reshape(experts, capacity)
    got_rows, got_pos = (
        lax.all_to_all(send_rows, "expert", split_axis=0, concat_axis=0, tiled=True),
        lax.all_to_all(send_pos, "expert", split_axis=0, concat_axis=0, tiled=True),
    )
    routed_one = got_rows.reshape(row_count, width)
    slot_pos = got_pos.reshape(row_count)
    query = weight_fold(routed_one, w_query[0]).astype(jnp.bfloat16)
    query_heads = query.reshape(row_count, HEADS, HEAD_DIM)

    def stat_step(carry_in, key_heads, value_heads, key_pos):
        highest, running = carry_in
        scores, allowed = masked_scores(query_heads, key_heads, slot_pos, key_pos)
        new_high = jnp.maximum(highest, jnp.max(jnp.where(allowed, scores, -1e30), axis=-1))
        running = running * jnp.exp(highest - new_high) + jnp.sum(
            jnp.where(allowed, jnp.exp(scores - new_high[:, :, None]), 0.0), axis=-1
        )
        return (new_high, running)

    highest, running = key_fold(
        kv_rows,
        stat_step,
        (
            jnp.full((HEADS, row_count), -1e30, jnp.float32),
            jnp.zeros((HEADS, row_count), jnp.float32),
        ),
    )
    log_norm = highest + jnp.log(running)

    def value_step(carry_in, key_heads, value_heads, key_pos):
        scores, allowed = masked_scores(query_heads, key_heads, slot_pos, key_pos)
        probabilities = jnp.where(allowed, jnp.exp(scores - log_norm[:, :, None]), 0.0).astype(
            jnp.bfloat16
        )
        return carry_in + jnp.einsum(
            "hrk,khd->rhd", probabilities, value_heads, preferred_element_type=jnp.float32
        )

    attended = key_fold(kv_rows, value_step, jnp.zeros((row_count, HEADS, HEAD_DIM), jnp.float32))
    attended = attended.reshape(row_count, QD).astype(jnp.bfloat16)
    branch_rows = weight_fold(attended, w_out[0]).astype(jnp.bfloat16)
    branch_back = to_home(branch_rows.reshape(experts, capacity, width))
    branch_pairs = collect_pairs(low_table_a, branch_back)
    residual_one = x_float + jnp.sum(shares_a[:, :, None] * branch_pairs, axis=1)
    scale_two = rms_scale(residual_one)
    normed_two = (residual_one * scale_two * norm2_gain).astype(jnp.bfloat16)
    shares_f, picked_f = pair_gates(
        jnp.dot(normed_two, ffn_router, preferred_element_type=jnp.float32),
        ffn_routes[0],
        live,
        experts,
    )
    table_f = route_table(ffn_routes[0], live_int, experts, capacity)
    low_table_f = table_f.astype(jnp.bfloat16)
    routed_two = to_owner(dispatch(low_table_f, normed_two, experts, capacity)).reshape(
        row_count, width
    )
    both = unit_forward(routed_two, w_in[0])
    hidden = (jax.nn.silu(both[:, :FF]) * both[:, FF:]).astype(jnp.bfloat16)
    down_rows = weight_fold(hidden, w_down[0]).astype(jnp.bfloat16)
    down_back = to_home(down_rows.reshape(experts, capacity, width))
    down_pairs = collect_pairs(low_table_f, down_back)
    mixed = jnp.sum(shares_f[:, :, None] * down_pairs, axis=1)
    layer_output = (live[:, None] * (residual_one + mixed)).astype(jnp.bfloat16)
    grad_out = output_grad[0].astype(jnp.float32) * live[:, None]
    pair_grad_f = jnp.sum(grad_out[:, None, :] * down_pairs, axis=-1)
    d_down = to_owner(spread_back(table_f, shares_f, grad_out, experts, capacity)).reshape(
        row_count, width
    )
    d_hidden = weight_back(d_down, w_down[0])
    gate_part = both[:, :FF]
    up_part = both[:, FF:]
    sigmoid_gate = jax.nn.sigmoid(gate_part)
    d_gate = d_hidden * up_part * sigmoid_gate * (1.0 + gate_part * (1.0 - sigmoid_gate))
    d_up = d_hidden * gate_part * sigmoid_gate
    d_gate_up = jnp.concatenate([d_gate, d_up], axis=1).astype(jnp.bfloat16)
    d_routed_two = unit_backward(d_gate_up, w_in[0]).astype(jnp.bfloat16)
    grad_w_in = unit_grad(d_gate_up, routed_two)
    grad_w_down = weight_grad(hidden, d_down)
    d_copy_two = to_home(d_routed_two.reshape(experts, capacity, width))
    dlog_f = logit_grad(shares_f, picked_f, pair_grad_f)
    d_normed_two = collect_sum(low_table_f, d_copy_two) + jnp.dot(
        dlog_f, ffn_router.astype(jnp.float32).T, precision=PRECISE
    )
    local_ffn_router = jnp.dot(normed_two.astype(jnp.float32).T, dlog_f, precision=PRECISE)
    d_mid, local_gain_two = norm_back(residual_one, scale_two, norm2_gain, d_normed_two)
    d_residual = grad_out + d_mid
    pair_grad_a = jnp.sum(d_residual[:, None, :] * branch_pairs, axis=-1)
    d_branch = to_owner(spread_back(table_a, shares_a, d_residual, experts, capacity)).reshape(
        row_count, width
    )
    d_attended = weight_back(d_branch, w_out[0]).astype(jnp.bfloat16)
    grad_w_out = weight_grad(attended, d_branch)
    delta_rows = jnp.sum(
        (d_attended.astype(jnp.float32) * attended.astype(jnp.float32)).reshape(
            row_count, HEADS, HEAD_DIM
        ),
        axis=-1,
    )
    delta_sum = delta_rows.T
    d_attended_heads = d_attended.reshape(row_count, HEADS, HEAD_DIM)

    def query_grad_step(carry_in, key_heads, value_heads, key_pos):
        scores, allowed = masked_scores(query_heads, key_heads, slot_pos, key_pos)
        probabilities = jnp.where(allowed, jnp.exp(scores - log_norm[:, :, None]), 0.0)
        d_prob = jnp.einsum(
            "rhd,khd->hrk", d_attended_heads, value_heads, preferred_element_type=jnp.float32
        )
        d_scores = (probabilities * (d_prob - delta_sum[:, :, None])).astype(jnp.bfloat16)
        return carry_in + jnp.einsum(
            "hrk,khd->rhd", d_scores, key_heads, preferred_element_type=jnp.float32
        )

    d_query_sum = key_fold(
        kv_rows, query_grad_step, jnp.zeros((row_count, HEADS, HEAD_DIM), jnp.float32)
    )
    d_query = (d_query_sum * HEAD_DIM ** (-0.5)).reshape(row_count, QD).astype(jnp.bfloat16)
    d_routed_one = weight_back(d_query, w_query[0]).astype(jnp.bfloat16)
    grad_w_query = weight_grad(routed_one, d_query)
    d_copy_one = to_home(d_routed_one.reshape(experts, capacity, width))
    own_keys = kv_rows[:, :QD].reshape(tokens, HEADS, HEAD_DIM)
    own_values = kv_rows[:, QD:].reshape(tokens, HEADS, HEAD_DIM)
    zeros_heads = jnp.zeros((tokens, HEADS, HEAD_DIM), jnp.float32)
    carried = (zeros_heads, zeros_heads)
    shard_piece = (
        lax.all_gather(query, ("expert", "context"), axis=0, tiled=True),
        lax.all_gather(d_attended, ("expert", "context"), axis=0, tiled=True),
        lax.all_gather(
            log_norm.T.astype(jnp.bfloat16), ("expert", "context"), axis=0, tiled=True
        ).astype(jnp.float32),
        lax.all_gather(
            delta_rows.astype(jnp.bfloat16), ("expert", "context"), axis=0, tiled=True
        ).astype(jnp.float32),
        lax.all_gather(slot_pos, ("expert", "context"), axis=0, tiled=True),
    )
    piece_len = shard_piece[0].shape[0]
    block_len = math.gcd(piece_len, row_count)

    def body_one_block(carry_in, element):
        query_part, grad_part, norm_part, delta_part, pos_part = element
        query_low = query_part.reshape(block_len, HEADS, HEAD_DIM)
        grad_low = grad_part.reshape(block_len, HEADS, HEAD_DIM)
        scores, allowed = masked_scores(query_low, own_keys, pos_part, position)
        probabilities = jnp.where(allowed, jnp.exp(scores - norm_part.T[:, :, None]), 0.0)
        d_prob = jnp.einsum(
            "rhd,khd->hrk", grad_low, own_values, preferred_element_type=jnp.float32
        )
        d_scores = (probabilities * (d_prob - delta_part.T[:, :, None])).astype(jnp.bfloat16)
        d_keys, d_values = carry_in
        d_keys = d_keys + jnp.einsum(
            "hrk,rhd->khd", d_scores, query_low, preferred_element_type=jnp.float32
        )
        d_values = d_values + jnp.einsum(
            "hrk,rhd->khd",
            probabilities.astype(jnp.bfloat16),
            grad_low,
            preferred_element_type=jnp.float32,
        )
        return ((d_keys, d_values), None)

    shaped = tuple(
        (
            member.reshape((piece_len // block_len, block_len) + member.shape[1:])
            for member in shard_piece
        )
    )
    carried, _ = lax.scan(body_one_block, carried, shaped)
    d_keys, d_values = carried
    d_kv = jnp.concatenate(
        [d_keys.reshape(tokens, QD) * HEAD_DIM ** (-0.5), d_values.reshape(tokens, QD)], axis=1
    ).astype(jnp.bfloat16)
    grad_w_kv = lax.psum(weight_grad(normed_one, d_kv).astype(jnp.bfloat16), "expert").astype(
        jnp.float32
    )
    dlog_a = logit_grad(shares_a, picked_a, pair_grad_a)
    d_normed_one = (
        collect_sum(low_table_a, d_copy_one)
        + weight_back(d_kv, w_kv)
        + jnp.dot(dlog_a, attn_router.astype(jnp.float32).T, precision=PRECISE)
    )
    local_attn_router = jnp.dot(normed_one.astype(jnp.float32).T, dlog_a, precision=PRECISE)
    d_first, local_gain_one = norm_back(x_float, scale_one, norm1_gain, d_normed_one)
    input_grad = d_residual + d_first
    gain_one_sum, gain_two_sum, router_a_sum, router_f_sum = lax.psum(
        (local_gain_one, local_gain_two, local_attn_router, local_ffn_router),
        ("expert", "context", "dp"),
    )
    return (
        layer_output[None],
        input_grad[None],
        gain_one_sum,
        gain_two_sum,
        router_a_sum,
        router_f_sum,
        grad_w_kv,
        grad_w_query[None],
        grad_w_out[None],
        grad_w_in[None],
        grad_w_down[None],
    )


MESH = pl.DeviceIdType.MESH
EVERY = ("dp", "expert", "context")
SHARE = ("context", "dp")

class Place:
    def __init__(self):
        self.e = lax.axis_index("expert")
        self.x = lax.axis_index("context")
        self.z = lax.axis_index("dp")
        self.own = (self.e, self.x)
        self.c = lax.rem(self.e, 2)
        self.sib = (self.e + 1 - 2 * self.c, self.x)
        self.cols = self.columns(self.e, self.x, self.c)
        self.sib_cols = self.columns(self.sib[0], self.x, 1 - self.c)

    def columns(self, e, x, c):
        first = (lax.rem(e + 2 * c, 4), lax.rem(x + 1 - c, 2))
        second = (lax.rem(e + 2 * (1 - c), 4), lax.rem(x + c, 2))
        return ((e, x), first, second, (lax.rem(e + 2, 4), 1 - x))

    def dev(self, col, z=None):
        return (col[0], col[1], self.z if z is None else z)

    def block(self, col, z):
        return z * 8 + col[0] * 2 + col[1]


def signal(barrier, dev):
    pl.semaphore_signal(barrier, inc=1, device_id=dev, device_id_type=MESH)


def greet(pc):
    barrier = pltpu.get_barrier_semaphore()
    for col in (pc.sib, pc.cols[1], pc.cols[2]):
        signal(barrier, pc.dev(col))
    pl.when(pc.z > 0)(lambda: signal(barrier, pc.dev(pc.own, pc.z - 1)))
    pl.when(pc.z < 3)(lambda: signal(barrier, pc.dev(pc.own, pc.z + 1)))
    pl.semaphore_wait(barrier, 3 + lax.div(pc.z + 3, 4) + lax.div(6 - pc.z, 4))


class Copies:
    def __init__(self, parts):
        self.parts = parts

    def start(self):
        for part in self.parts:
            part.start()

    def wait_send(self):
        for part in self.parts:
            part.wait_send()

    def wait_recv(self):
        for part in self.parts:
            part.wait_recv()


def remote(src, dst, send, recv, dev):
    return pltpu.make_async_remote_copy(
        src_ref=src, dst_ref=dst, send_sem=send, recv_sem=recv, device_id=dev, device_id_type=MESH
    )


def when_in(cond, run):
    if cond is True:
        run()
    else:
        pl.when(cond)(run)


class Gather:
    sems = ((), (2, 4), (2, 4), (7,), (7,), (2, 7), (2, 7), (4, 7), (4, 7))

    def __init__(self, pc, ins, outs, sems):
        self.pc, self.ins, self.outs = pc, ins, outs
        self.loc, self.zs, self.zr, self.fs, self.fr, self.ss, self.sr, self.bs, self.br = sems

    @classmethod
    def scratch(cls, payloads):
        return [pltpu.SemaphoreType.DMA((payloads,) + shape) for shape in cls.sems]

    def copies(self, src_own, blk, send, recv, at, dev):
        return Copies(
            [
                remote(
                    self.ins[p] if src_own else self.outs[p].at[blk],
                    self.outs[p].at[blk],
                    send.at[(p,) + at],
                    recv.at[(p,) + at],
                    dev,
                )
                for p in range(len(self.ins))
            ]
        )

    def hop(self, col, d, kind):
        pc = self.pc
        blk = pc.block(pc.cols[col], pc.z + d)
        own = col == 0 and d == 0
        if kind == "f":
            return self.copies(own, blk, self.fs, self.fr, (d + 3,), pc.dev(pc.cols[1]))
        if kind == "s":
            return self.copies(own, blk, self.ss, self.sr, (col, d + 3), pc.dev(pc.cols[2]))
        return self.copies(own, blk, self.bs, self.br, (col, d + 3), pc.dev(pc.sib))

    def line(self, d, up):
        pc = self.pc
        dev = pc.dev(pc.own, pc.z + 1 if up else pc.z - 1)
        blk = pc.block(pc.own, pc.z + d)
        return self.copies(d == 0, blk, self.zs, self.zr, (0 if up else 1, abs(d)), dev)

    def arrival(self, col, d, recv, at, dev):
        blk = self.pc.block(col, self.pc.z + d)
        return self.copies(False, blk, recv, recv, at, dev)

    def present(self, d):
        return True if d == 0 else (self.pc.z + d >= 0) & (self.pc.z + d <= 3)

    def keep_own(self):
        pc = self.pc
        return [
            pltpu.make_async_copy(
                self.ins[p], self.outs[p].at[pc.block(pc.own, pc.z)], self.loc.at[p]
            )
            for p in range(len(self.ins))
        ]

    def start(self):
        for copy in self.keep_own():
            copy.start()

    def own_line(self, d):
        pc = self.pc

        def run():
            if d < 0:
                below = pc.dev(pc.own, pc.z - 1)
                self.arrival(pc.own, d, self.zr, (0, -d - 1), below).wait_recv()
            if d > 0:
                above = pc.dev(pc.own, pc.z + 1)
                self.arrival(pc.own, d, self.zr, (1, d - 1), above).wait_recv()
            if d <= 0:
                pl.when(pc.z < 3)(lambda: self.line(d, True).start())
            if d >= 0:
                pl.when(pc.z > 0)(lambda: self.line(d, False).start())
            for kind in ("f", "s", "b"):
                self.hop(0, d, kind).start()

        when_in(self.present(d), run)

    def first_col(self, d):
        pc = self.pc

        def run():
            self.arrival(pc.cols[1], d, self.fr, (d + 3,), pc.dev(pc.cols[1])).wait_recv()
            self.hop(1, d, "s").start()
            self.hop(1, d, "b").start()

        when_in(self.present(d), run)

    def last_cols(self, d):
        pc = self.pc

        def run():
            for col, sent in ((2, 0), (3, 1)):
                dev = pc.dev(pc.cols[2])
                self.arrival(pc.cols[col], d, self.sr, (sent, d + 3), dev).wait_recv()
                self.hop(col, d, "b").start()

        when_in(self.present(d), run)

    def finish(self, d):
        pc = self.pc

        def run():
            for col in range(4):
                dev = pc.dev(pc.sib)
                self.arrival(pc.sib_cols[col], d, self.br, (col, d + 3), dev).wait_recv()
            self.hop(0, d, "f").wait_send()
            for col in (0, 1):
                self.hop(col, d, "s").wait_send()
            for col in range(4):
                self.hop(col, d, "b").wait_send()
            if d <= 0:
                pl.when(pc.z < 3)(lambda: self.line(d, True).wait_send())
            if d >= 0:
                pl.when(pc.z > 0)(lambda: self.line(d, False).wait_send())

        when_in(self.present(d), run)

    def end(self):
        for copy in self.keep_own():
            copy.wait()

    def events(self):
        steps = [(self.own_line, 0)]
        for s in (1, 2, 3):
            steps += [(self.own_line, -s), (self.own_line, s)]
            steps += [(self.first_col, d) for d in sorted({1 - s, s - 1})]
        steps += [(self.first_col, -3), (self.first_col, 3)]
        order = (0, -1, 1, -2, 2, -3, 3)
        steps += [(self.last_cols, d) for d in order] + [(self.finish, d) for d in order]
        return [lambda run=run, d=d: run(d) for run, d in steps]


def gather_kernel(count, *refs):
    pc = Place()
    gather = Gather(pc, refs[:count], refs[count : 2 * count], refs[2 * count :])
    gather.start()
    greet(pc)
    for event in gather.events():
        event()
    gather.end()


def gather_all(blocks, cid):
    count = len(blocks)
    return pl.pallas_call(
        functools.partial(gather_kernel, count),
        out_shape=[jax.ShapeDtypeStruct((32,) + b.shape, b.dtype) for b in blocks],
        in_specs=[pl.BlockSpec(memory_space=pltpu.VMEM)] * count,
        out_specs=[pl.BlockSpec(memory_space=pl.ANY)] * count,
        scratch_shapes=Gather.scratch(count),
        compiler_params=pltpu.CompilerParams(collective_id=cid, has_side_effects=True),
        name="gather_all",
    )(*blocks)


class Scatter:
    sems = ((4, 4), (4, 4), (4, 4), (4, 2), (4, 2), (4,), (4,), (2, 4), (2, 4))

    def __init__(self, pc, ins, bufs, sems):
        self.pc, self.ins = pc, ins
        count = len(ins)
        self.acc, self.sib, self.sec, self.fst, self.zin = (
            bufs[i * count : (i + 1) * count] for i in range(5)
        )
        self.ld, self.bs, self.br, self.ss, self.sr, self.fs, self.fr, self.zs, self.zr = sems
        inner = lax.rem(lax.div(pc.z + 1, 2), 2)
        low = 1 - lax.div(pc.z, 2)

        def group(k):
            v = (1 - inner) * k + inner * (0, 1, 3, 2)[k]
            return low * (3 - v) + (1 - low) * v

        self.group = group

    @classmethod
    def scratch(cls, blocks):
        bufs = []
        for lead in ((4, 4), (4, 4), (4, 2), (4,), (2, 4)):
            bufs += [pltpu.VMEM(lead + shape, dtype) for shape, dtype in blocks]
        return bufs + [pltpu.SemaphoreType.DMA((len(blocks),) + s) for s in cls.sems]

    def copies(self, src, dst, send, recv, sent_at, got_at, dev):
        return Copies(
            [
                remote(src(p), dst(p), send.at[(p,) + sent_at], recv.at[(p,) + got_at], dev)
                for p in range(len(self.ins))
            ]
        )

    def loads(self, k, col):
        pc = self.pc
        blk = pc.block(pc.cols[col], self.group(k))
        return [
            pltpu.make_async_copy(self.ins[p].at[blk], self.acc[p].at[k, col], self.ld.at[p, k, col])
            for p in range(len(self.ins))
        ]

    def to_sib(self, k, col):
        pc = self.pc
        blk = pc.block(pc.sib_cols[col], self.group(k))
        return self.copies(
            lambda p: self.ins[p].at[blk], lambda p: self.sib[p].at[k, col],
            self.bs, self.br, (k, col), (k, col), pc.dev(pc.sib),
        )

    def to_second(self, k, j):
        pc = self.pc
        return self.copies(
            lambda p: self.acc[p].at[k, 2 + j], lambda p: self.sec[p].at[k, j],
            self.ss, self.sr, (k, j), (k, j), pc.dev(pc.cols[2]),
        )

    def to_first(self, k):
        pc = self.pc
        return self.copies(
            lambda p: self.acc[p].at[k, 1], lambda p: self.fst[p].at[k],
            self.fs, self.fr, (k,), (k,), pc.dev(pc.cols[1]),
        )

    def to_z(self, k, up):
        pc, g, i = self.pc, self.group(k), 0 if up else 1
        return self.copies(
            lambda p: self.acc[p].at[k, 0], lambda p: self.zin[p].at[i, g],
            self.zs, self.zr, (i, k), (i, g), pc.dev(pc.own, pc.z + 1 if up else pc.z - 1),
        )

    def from_z(self, g, i):
        pc = self.pc
        return self.copies(
            lambda p: self.acc[p].at[0, 0], lambda p: self.zin[p].at[i, g],
            self.zs, self.zr, (i, 0), (i, g), pc.dev(pc.own, pc.z - 1 if i == 0 else pc.z + 1),
        )

    def add(self, k, col, others):
        for acc, other in zip(self.acc, others):
            rows, step = acc.shape[2], min(16, acc.shape[2])

            def body(i, carry, acc=acc, other=other, step=step):
                r = pl.ds(pl.multiple_of(i * step, step), step)
                both = acc[k, col, r, :].astype(jnp.float32) + other[r, :].astype(jnp.float32)
                acc[k, col, r, :] = both.astype(acc.dtype)
                return carry

            lax.fori_loop(0, rows // step, body, 0)

    def start_loads(self):
        for k in range(4):
            for col in (2, 3, 1, 0):
                for copy in self.loads(k, col):
                    copy.start()

    def start(self):
        for k in range(4):
            for col in (2, 3, 1, 0):
                self.to_sib(k, col).start()

    def join(self, k, col):
        for copy in self.loads(k, col):
            copy.wait()
        self.to_sib(k, col).wait_recv()
        self.add(k, col, [buf.at[k, col] for buf in self.sib])

    def stage_a(self, k):
        for j in (0, 1):
            self.join(k, 2 + j)
            self.to_second(k, j).start()

    def stage_b(self, k):
        self.join(k, 1)
        self.to_second(k, 1).wait_recv()
        self.add(k, 1, [buf.at[k, 1] for buf in self.sec])
        self.to_first(k).start()
        self.join(k, 0)

    def stage_c(self, k):
        z = self.pc.z
        self.to_second(k, 0).wait_recv()
        self.add(k, 0, [buf.at[k, 0] for buf in self.sec])
        self.to_first(k).wait_recv()
        self.add(k, 0, [buf.at[k] for buf in self.fst])
        g = self.group(k)

        def arrive(i):
            self.from_z(g, i).wait_recv()
            self.add(k, 0, [buf.at[i, g] for buf in self.zin])

        def upward():
            pl.when(z > 0)(lambda: arrive(0))
            self.to_z(k, True).start()

        def downward():
            pl.when(z < 3)(lambda: arrive(1))
            self.to_z(k, False).start()

        if k < 3:
            pl.when(g > z)(upward)
            pl.when(g < z)(downward)
        else:
            pl.when(z > 0)(lambda: arrive(0))
            pl.when(z < 3)(lambda: arrive(1))

    def events(self):
        a, b, c = self.stage_a, self.stage_b, self.stage_c
        steps = [(a, 0), (a, 1), (b, 0), (a, 2), (b, 1), (c, 0), (a, 3), (b, 2), (c, 1), (b, 3)]
        return [lambda run=run, k=k: run(k) for run, k in steps + [(c, 2), (c, 3)]]

    def end(self):
        z = self.pc.z
        for k in range(4):
            for col in range(4):
                self.to_sib(k, col).wait_send()
            for j in (0, 1):
                self.to_second(k, j).wait_send()
            self.to_first(k).wait_send()
            if k < 3:
                pl.when(self.group(k) > z)(lambda: self.to_z(k, True).wait_send())
                pl.when(self.group(k) < z)(lambda: self.to_z(k, False).wait_send())


def scatter_kernel(count, *refs):
    pc = Place()
    outs = refs[count : 2 * count]
    scatter = Scatter(pc, refs[:count], refs[2 * count : 7 * count], refs[7 * count :])
    scatter.start_loads()
    greet(pc)
    scatter.start()
    for event in scatter.events():
        event()
    for p in range(count):
        outs[p][...] = scatter.acc[p][3, 0]
    scatter.end()


def scatter_all(wholes, cid):
    count = len(wholes)
    blocks = [(w.shape[1:], w.dtype) for w in wholes]
    return pl.pallas_call(
        functools.partial(scatter_kernel, count),
        out_shape=[jax.ShapeDtypeStruct(*b) for b in blocks],
        in_specs=[pl.BlockSpec(memory_space=pl.ANY)] * count,
        out_specs=[pl.BlockSpec(memory_space=pltpu.VMEM)] * count,
        scratch_shapes=Scatter.scratch(blocks),
        compiler_params=pltpu.CompilerParams(
            collective_id=cid, has_side_effects=True, vmem_limit_bytes=48 << 20
        ),
        name="scatter_all",
    )(*wholes)


def sum_kernel(v_ref, out_ref, cur, got, lines, send, recv, zsend, zrecv):
    pc = Place()
    z = pc.z
    near = (pc.sib, (pc.e, 1 - pc.x), (lax.rem(pc.e + 2, 4), pc.x))
    barrier = pltpu.get_barrier_semaphore()
    for col in near:
        signal(barrier, pc.dev(col))
    for d in (1, 2, 3):
        signal(barrier, pc.dev(pc.own, lax.rem(z + d, 4)))
    pl.semaphore_wait(barrier, 6)
    for s, col in enumerate(near):
        src = v_ref if s == 0 else cur.at[s - 1]
        copy = remote(src, got.at[s], send.at[s], recv.at[s], pc.dev(col))
        copy.start()
        copy.wait_recv()
        cur[s] = src[...] + got[s]

    def along(d):
        there = lax.rem(z + d, 4)
        return remote(cur.at[2], lines.at[z], zsend.at[d], zrecv.at[z], pc.dev(pc.own, there))

    for d in (1, 2, 3):
        along(d).start()
    for d in (1, 2, 3):
        source = lax.rem(z + d, 4)
        remote(
            cur.at[2], lines.at[source], zsend.at[0], zrecv.at[source], pc.dev(pc.own, source)
        ).wait_recv()
    lines[z] = cur[2]
    out_ref[...] = ((lines[0] + lines[1]) + lines[2]) + lines[3]
    for s, col in enumerate(near):
        src = v_ref if s == 0 else cur.at[s - 1]
        remote(src, got.at[s], send.at[s], recv.at[s], pc.dev(col)).wait_send()
    for d in (1, 2, 3):
        along(d).wait_send()


def sum_all(v, cid):
    D = pltpu.SemaphoreType.DMA
    return pl.pallas_call(
        sum_kernel,
        out_shape=jax.ShapeDtypeStruct(v.shape, v.dtype),
        in_specs=[pl.BlockSpec(memory_space=pltpu.VMEM)],
        out_specs=pl.BlockSpec(memory_space=pltpu.VMEM),
        scratch_shapes=[
            pltpu.VMEM((3,) + v.shape, v.dtype),
            pltpu.VMEM((3,) + v.shape, v.dtype),
            pltpu.VMEM((4,) + v.shape, v.dtype),
            D((3,)), D((3,)), D((4,)), D((4,)),
        ],
        compiler_params=pltpu.CompilerParams(collective_id=cid, has_side_effects=True),
        name="sum_all",
    )(v)


def attend_kernel(qkv_ref, att_ref, lse_ref):
    length = qkv_ref.shape[0]
    tile = 256
    heads = att_ref.shape[1] // HEAD_DIM
    for head in range(heads):
        at = lambda part: pl.ds((part * heads + head) * HEAD_DIM, HEAD_DIM)
        for first in range(0, length, tile):
            last = first + tile
            q = qkv_ref[pl.ds(first, tile), at(0)]
            k = qkv_ref[pl.ds(0, last), at(1)]
            v = qkv_ref[pl.ds(0, last), at(2)]
            scores = lax.dot_general(
                k, q, (((1,), (1,)), ((), ())), preferred_element_type=jnp.float32
            ) * HEAD_DIM ** (-0.5)
            key_pos = lax.broadcasted_iota(jnp.int32, scores.shape, 0)
            query_pos = first + lax.broadcasted_iota(jnp.int32, scores.shape, 1)
            scores = jnp.where(key_pos <= query_pos, scores, -1e30)
            highest = jnp.max(scores, axis=0, keepdims=True)
            exponent = jnp.exp(scores - highest)
            total = jnp.sum(exponent, axis=0, keepdims=True)
            mixed = lax.dot_general(
                v,
                exponent.astype(jnp.bfloat16),
                (((0,), (0,)), ((), ())),
                preferred_element_type=jnp.float32,
            )
            mixed = mixed * (1.0 / total)
            att_ref[pl.ds(first, tile), pl.ds(head * HEAD_DIM, HEAD_DIM)] = mixed.T.astype(
                jnp.bfloat16
            )
            lse_ref[0, pl.ds(head, 1), pl.ds(first, tile)] = highest + jnp.log(total)


def attend(qkv, slots):
    rows, width = qkv.shape
    length = rows // slots
    out = width // 3
    return pl.pallas_call(
        attend_kernel,
        grid=(slots,),
        out_shape=(
            jax.ShapeDtypeStruct((rows, out), jnp.bfloat16),
            jax.ShapeDtypeStruct((slots, out // HEAD_DIM, length), jnp.float32),
        ),
        in_specs=[pl.BlockSpec((length, width), lambda s: (s, 0))],
        out_specs=(
            pl.BlockSpec((length, out), lambda s: (s, 0)),
            pl.BlockSpec((1, out // HEAD_DIM, length), lambda s: (s, 0, 0)),
        ),
        compiler_params=pltpu.CompilerParams(vmem_limit_bytes=48 << 20),
        name="attend",
    )(qkv)


def attend_back_kernel(qkv_ref, du_ref, lse_ref, gate_ref, dqkv_ref, dgate_ref, dk_acc, dv_acc):
    length = qkv_ref.shape[0]
    tile = 256
    heads = du_ref.shape[1] // HEAD_DIM
    scale = HEAD_DIM ** (-0.5)
    for head in range(heads):
        at = lambda part: pl.ds((part * heads + head) * HEAD_DIM, HEAD_DIM)
        dk_acc[...] = jnp.zeros_like(dk_acc)
        dv_acc[...] = jnp.zeros_like(dv_acc)
        for first in range(0, length, tile):
            last = first + tile
            q = qkv_ref[pl.ds(first, tile), at(0)]
            k = qkv_ref[pl.ds(0, last), at(1)]
            v = qkv_ref[pl.ds(0, last), at(2)]
            du = du_ref[pl.ds(first, tile), pl.ds(head * HEAD_DIM, HEAD_DIM)]
            gate = gate_ref[0, :, pl.ds(first, tile)]
            lse = lse_ref[0, pl.ds(head, 1), pl.ds(first, tile)]
            scores = (
                lax.dot_general(k, q, (((1,), (1,)), ((), ())), preferred_element_type=jnp.float32)
                * scale
            )
            key_pos = lax.broadcasted_iota(jnp.int32, scores.shape, 0)
            query_pos = first + lax.broadcasted_iota(jnp.int32, scores.shape, 1)
            probs = jnp.where(key_pos <= query_pos, jnp.exp(scores - lse), 0.0)
            d_prob = lax.dot_general(
                v, du, (((1,), (1,)), ((), ())), preferred_element_type=jnp.float32
            )
            along = jnp.sum(probs * d_prob, axis=0, keepdims=True)
            dgate_ref[0, pl.ds(head, 1), pl.ds(first, tile)] = along
            shared = probs * gate
            d_scores = (shared * (d_prob - along)).astype(jnp.bfloat16)
            dq = lax.dot_general(
                d_scores, k, (((0,), (0,)), ((), ())), preferred_element_type=jnp.float32
            )
            dqkv_ref[pl.ds(first, tile), at(0)] = (dq * scale).astype(jnp.bfloat16)
            dk_acc[pl.ds(0, last), :] += jnp.dot(d_scores, q, preferred_element_type=jnp.float32)
            dv_acc[pl.ds(0, last), :] += jnp.dot(
                shared.astype(jnp.bfloat16), du, preferred_element_type=jnp.float32
            )
        dqkv_ref[:, at(1)] = (dk_acc[...] * scale).astype(jnp.bfloat16)
        dqkv_ref[:, at(2)] = dv_acc[...].astype(jnp.bfloat16)


def attend_back(qkv, du, lse, gate, slots):
    rows, width = qkv.shape
    length = rows // slots
    out = width // 3
    heads = out // HEAD_DIM
    return pl.pallas_call(
        attend_back_kernel,
        grid=(slots,),
        out_shape=(
            jax.ShapeDtypeStruct((rows, width), jnp.bfloat16),
            jax.ShapeDtypeStruct((slots, heads, length), jnp.float32),
        ),
        in_specs=[
            pl.BlockSpec((length, width), lambda s: (s, 0)),
            pl.BlockSpec((length, out), lambda s: (s, 0)),
            pl.BlockSpec((1, heads, length), lambda s: (s, 0, 0)),
            pl.BlockSpec((1, 1, length), lambda s: (s, 0, 0)),
        ],
        out_specs=(
            pl.BlockSpec((length, width), lambda s: (s, 0)),
            pl.BlockSpec((1, heads, length), lambda s: (s, 0, 0)),
        ),
        scratch_shapes=[
            pltpu.VMEM((length, HEAD_DIM), jnp.float32),
            pltpu.VMEM((length, HEAD_DIM), jnp.float32),
        ],
        compiler_params=pltpu.CompilerParams(vmem_limit_bytes=48 << 20),
        name="attend_back",
    )(qkv, du, lse, gate)


def as_rows(*columns):
    rows = jnp.concatenate([c.T for c in columns], axis=0)
    return jnp.pad(rows, ((0, -rows.shape[0] % 8), (0, 0)))


def expert_rows(per_block, experts):
    place = (jnp.arange(8) == lax.axis_index("expert")).astype(per_block.dtype)
    return per_block[:, None, :] * place[None, :, None]


def placed_weights(
    layer_input,
    output_grad,
    lengths,
    attn_routes,
    ffn_routes,
    norm1_gain,
    norm2_gain,
    attn_router,
    ffn_router,
    w_kv,
    w_query,
    w_out,
    w_in,
    w_down,
):
    f32, low = jnp.float32, jnp.bfloat16
    tokens, width = layer_input.shape[1:]
    experts = lax.axis_size("expert")
    contexts = lax.axis_size("context")
    slots = lax.axis_size("dp")
    shares = contexts * slots
    devices = experts * shares
    own_expert = lax.axis_index("expert")
    capacity = tokens * TOP // experts + tokens // 32
    room = -(-capacity // 8) * 8

    position = lax.axis_index(("expert", "context")) * tokens + jnp.arange(tokens, dtype=jnp.int32)
    live = (position < lengths[0]).astype(f32)
    x_float = layer_input[0].astype(f32)
    scale_one = rms_scale(x_float)
    normed_one = (x_float * scale_one * norm1_gain).astype(low)
    grad_out = output_grad[0].astype(f32) * live[:, None]

    kv_parts = w_kv.reshape(-1, 2, shares, QD // shares).transpose(0, 2, 1, 3)
    qkv_parts = jnp.concatenate(
        [w_query[0].reshape(-1, shares, QD // shares), kv_parts.reshape(kv_parts.shape[0], shares, -1)],
        axis=2,
    )
    piece = qkv_parts.shape[2]
    w_qkv = lax.all_to_all(
        qkv_parts.reshape(-1, shares * piece), SHARE, split_axis=1, concat_axis=0, tiled=True
    )

    shares_a, picked_a = pair_gates(
        jnp.dot(normed_one, attn_router, preferred_element_type=f32), attn_routes[0], live, experts
    )
    gates_a = jnp.sum(shares_a[:, :, None] * picked_a, axis=1)
    named_f = jnp.sum(
        (ffn_routes[0][:, :, None] == jnp.arange(experts, dtype=jnp.int32)).astype(f32), axis=1
    )
    named_f = named_f * live[:, None]
    all_one, aux = gather_all([normed_one, as_rows(gates_a, named_f)], 0)
    all_one = all_one.reshape(-1, width)
    gate_a = lax.dynamic_index_in_dim(aux, own_expert, axis=1, keepdims=False)
    named = lax.dynamic_index_in_dim(aux, experts + own_expert, axis=1, keepdims=False)
    all_one, own_in, own_down = lax.optimization_barrier((all_one, w_in[0], w_down[0]))
    w_pair = lax.all_to_all(own_in, "context", split_axis=0, concat_axis=0, tiled=True)
    share = lax.axis_index(SHARE)
    moves = [(s, (s % contexts) * slots + s // contexts) for s in range(shares)]
    stays = functools.reduce(jnp.logical_or, [share == s for s, d in moves if s == d])
    w_unit = lax.ppermute(own_down, SHARE, [(s, d) for s, d in moves if s != d])
    w_unit = jnp.where(stays, own_down, w_unit)
    units = w_unit.shape[0]
    qkv = jnp.dot(all_one, w_qkv, preferred_element_type=f32).astype(low)
    attended, lse = attend(qkv, slots)
    gated = (attended.astype(f32) * gate_a.reshape(-1, 1)).astype(low)
    h1_part = jnp.dot(gated, w_out[0], preferred_element_type=f32).astype(low)
    (h1_sum,) = scatter_all([h1_part.reshape(devices, tokens, width)], 1)
    residual_one = x_float + h1_sum.astype(f32)

    scale_two = rms_scale(residual_one)
    normed_two = (residual_one * scale_two * norm2_gain).astype(low)
    shares_f, picked_f = pair_gates(
        jnp.dot(normed_two, ffn_router, preferred_element_type=f32), ffn_routes[0], live, experts
    )
    gates_f = jnp.sum(shares_f[:, :, None] * picked_f, axis=1)
    all_two, aux = gather_all([normed_two, as_rows(gates_f)], 2)
    gate_f = lax.dynamic_index_in_dim(aux, own_expert, axis=1, keepdims=False)
    all_two, grad_low = lax.optimization_barrier((all_two, grad_out.astype(low)))
    (all_grad,) = gather_all([grad_low], 7)
    earlier = (jnp.arange(tokens)[:, None] < jnp.arange(tokens)[None, :]).astype(f32)
    rank = jnp.dot(named, earlier, preferred_element_type=f32)
    table = jnp.where(
        rank[:, None, :] == jnp.arange(room, dtype=f32)[None, :, None], named[:, None, :], 0.0
    )
    low_table = table.astype(low)

    def pick(whole):
        rows = jnp.einsum(
            "bst,btd->bsd",
            low_table,
            whole,
            preferred_element_type=f32,
        )
        return rows.astype(low).reshape(devices * room, width)

    def put(rows):
        whole = jnp.einsum(
            "bst,bsd->btd", low_table, rows.reshape(devices, room, width), preferred_element_type=f32
        )
        return whole.astype(low)

    row_gate = jnp.sum(table * gate_f[:, None, :], axis=2).reshape(-1, 1)
    routed = pick(all_two)
    both = lax.dot_general(routed, w_pair, (((1,), (1,)), ((), ())), preferred_element_type=f32)
    gate_part, up_part = both[:, :units], both[:, units:]
    sigmoid_gate = jax.nn.sigmoid(gate_part)
    hidden_f = gate_part * sigmoid_gate * up_part
    hidden = hidden_f.astype(low)
    down = (jnp.dot(hidden, w_unit, preferred_element_type=f32) * row_gate).astype(low)
    (mixed,) = scatter_all([put(down)], 3)
    layer_output = (live[:, None] * (residual_one + mixed.astype(f32))).astype(low)

    d_rows = pick(all_grad)
    d_plain = lax.dot_general(d_rows, w_unit, (((1,), (1,)), ((), ())), preferred_element_type=f32)
    row_sums = jnp.sum(d_plain * hidden.astype(f32), axis=1).reshape(devices, room)
    dgate_part = expert_rows(jnp.sum(table * row_sums[:, :, None], axis=1), experts)
    d_hidden = d_plain * row_gate
    d_gate = d_hidden * up_part * sigmoid_gate * (1.0 + gate_part * (1.0 - sigmoid_gate))
    d_up = d_hidden * gate_part * sigmoid_gate
    d_both = jnp.concatenate([d_gate, d_up], axis=1).astype(low)
    d_two_part = put(jnp.dot(d_both, w_pair, preferred_element_type=f32).astype(low))
    grad_unit = lax.dot_general(
        (hidden.astype(f32) * row_gate).astype(low),
        d_rows,
        (((0,), (0,)), ((), ())),
        preferred_element_type=f32,
    )
    grad_pair = lax.dot_general(
        d_both, routed, (((0,), (0,)), ((), ())), preferred_element_type=f32
    )
    grad_w_in = lax.all_to_all(
        grad_pair.astype(low), "context", split_axis=0, concat_axis=0, tiled=True
    ).astype(f32)
    grad_moved = lax.ppermute(grad_unit.astype(low), SHARE, [(d, s) for s, d in moves if s != d])
    grad_w_down = jnp.where(stays, grad_unit.astype(low), grad_moved).astype(f32)
    d_two_sum, dgate_f = scatter_all([d_two_part, dgate_part], 4)
    dgate_f = dgate_f[:experts].T
    dlog_f = gates_f * (dgate_f - jnp.sum(gates_f * dgate_f, axis=1, keepdims=True))
    d_normed_two = d_two_sum.astype(f32) + jnp.dot(
        dlog_f, ffn_router.astype(f32).T, precision=PRECISE
    )
    local_ffn_router = jnp.dot(dlog_f.T, normed_two.astype(f32), precision=PRECISE)
    d_mid, local_gain_two = norm_back(residual_one, scale_two, norm2_gain, d_normed_two)
    d_residual = grad_out + d_mid

    (all_mid,) = gather_all([d_residual.astype(low)], 5)
    all_mid = all_mid.reshape(-1, width)
    d_att = lax.dot_general(
        all_mid, w_out[0], (((1,), (1,)), ((), ())), preferred_element_type=f32
    ).astype(low)
    d_qkv, head_sums = attend_back(
        qkv, d_att, lse, gate_a.reshape(slots, 1, -1), slots
    )
    grad_w_out = lax.dot_general(
        gated, all_mid, (((0,), (0,)), ((), ())), preferred_element_type=f32
    )
    dgate_part = expert_rows(jnp.sum(head_sums, axis=1).reshape(devices, tokens), experts)
    d_one_part = lax.dot_general(
        d_qkv, w_qkv, (((1,), (1,)), ((), ())), preferred_element_type=f32
    ).astype(low)
    grad_qkv = lax.dot_general(
        all_one, d_qkv, (((0,), (0,)), ((), ())), preferred_element_type=f32
    ).astype(low)
    grad_parts = lax.all_to_all(grad_qkv, SHARE, split_axis=0, concat_axis=1, tiled=True)
    grad_parts = grad_parts.reshape(-1, shares, piece)
    grad_w_query = grad_parts[:, :, : QD // shares].reshape(-1, QD).astype(f32)
    kv_grads = grad_parts[:, :, QD // shares :].reshape(-1, shares, 2, QD // shares)
    grad_w_kv = lax.psum(kv_grads.transpose(0, 2, 1, 3).reshape(-1, 2 * QD), "expert").astype(f32)
    d_one_sum, dgate_a = scatter_all([d_one_part.reshape(devices, tokens, width), dgate_part], 6)
    dgate_a = dgate_a[:experts].T
    dlog_a = gates_a * (dgate_a - jnp.sum(gates_a * dgate_a, axis=1, keepdims=True))
    d_normed_one = d_one_sum.astype(f32) + jnp.dot(
        dlog_a, attn_router.astype(f32).T, precision=PRECISE
    )
    local_attn_router = jnp.dot(dlog_a.T, normed_one.astype(f32), precision=PRECISE)
    d_first, local_gain_one = norm_back(x_float, scale_one, norm1_gain, d_normed_one)
    input_grad = d_residual + d_first
    sums = sum_all(
        jnp.concatenate(
            [local_gain_one[None], local_gain_two[None], local_attn_router, local_ffn_router]
        ).reshape(-1, HEAD_DIM),
        8,
    ).reshape(-1, width)
    gain_one_sum, gain_two_sum = sums[0], sums[1]
    router_a_sum, router_f_sum = sums[2 : 2 + experts].T, sums[2 + experts :].T
    return (
        layer_output[None],
        input_grad[None],
        gain_one_sum,
        gain_two_sum,
        router_a_sum,
        router_f_sum,
        grad_w_kv,
        grad_w_query[None],
        grad_w_out[None],
        grad_w_in[None],
        grad_w_down[None],
    )


def fits_in_place(mesh):
    sizes = (mesh.shape["expert"], mesh.shape["context"], mesh.shape["dp"])
    return sizes == (4, 2, 4)


def solution(mesh):
    placed = (
        P("dp", ("expert", "context"), None),
        P("dp", ("expert", "context"), None),
        P("dp"),
        P("dp", ("expert", "context"), None),
        P("dp", ("expert", "context"), None),
        P(),
        P(),
        P(),
        P(),
        P(("context", "dp"), None),
        P("expert", ("context", "dp"), None),
        P("expert", ("context", "dp"), None),
        P("expert", ("context", "dp"), None),
        P("expert", ("context", "dp"), None),
    )
    return jax.shard_map(
        placed_weights if fits_in_place(mesh) else gathered_weights,
        mesh=mesh,
        in_specs=placed,
        out_specs=(
            P("dp", ("expert", "context"), None),
            P("dp", ("expert", "context"), None),
            P(),
            P(),
            P(),
            P(),
            P(("context", "dp"), None),
            P("expert", ("context", "dp"), None),
            P("expert", ("context", "dp"), None),
            P("expert", ("context", "dp"), None),
            P("expert", ("context", "dp"), None),
        ),
        check_vma=False,
    )
```

```python
import functools
import math

import jax
import jax.numpy as jnp
from jax import lax
from jax.experimental import pallas as pl
from jax.experimental.pallas import tpu as pltpu
from jax.sharding import PartitionSpec as P


HEADS = 16
HEAD_DIM = 128
FF = 5632
TOP = 2
QD = 2048


EPSILON = 1e-06
PRECISE = lax.Precision.HIGHEST


def rms_scale(value):
    return lax.rsqrt(jnp.mean(value * value, axis=-1, keepdims=True) + EPSILON)


def norm_back(value, scale, gain, grad_normed):
    weighted = grad_normed * gain
    d_gain = jnp.sum(grad_normed * value * scale, axis=0)
    d_value = scale * weighted - value * scale**3 * jnp.mean(
        weighted * value, axis=-1, keepdims=True
    )
    return (d_value, d_gain)


def weight_fold(left_rows, weight):
    return jnp.dot(
        left_rows,
        lax.all_gather(weight, ("context", "dp"), axis=0, tiled=True),
        preferred_element_type=jnp.float32,
    )


def weight_back(gradient, weight):
    return lax.dot_general(
        gradient,
        lax.all_gather(weight, ("context", "dp"), axis=0, tiled=True),
        (((1,), (1,)), ((), ())),
        preferred_element_type=jnp.float32,
    )


def weight_grad(left_rows, gradient):
    return lax.psum_scatter(
        lax.dot_general(
            left_rows, gradient, (((0,), (0,)), ((), ())), preferred_element_type=jnp.float32
        ).astype(jnp.bfloat16),
        ("context", "dp"),
        scatter_dimension=0,
        tiled=True,
    ).astype(jnp.float32)


def unit_forward(left_rows, weight):
    return lax.dot_general(
        left_rows,
        lax.all_gather(weight, ("context", "dp"), axis=0, tiled=True),
        (((1,), (1,)), ((), ())),
        preferred_element_type=jnp.float32,
    )


def unit_backward(gradient, weight):
    return jnp.dot(
        gradient,
        lax.all_gather(weight, ("context", "dp"), axis=0, tiled=True),
        preferred_element_type=jnp.float32,
    )


def unit_grad(gradient, left_rows):
    return lax.psum_scatter(
        lax.dot_general(
            gradient, left_rows, (((0,), (0,)), ((), ())), preferred_element_type=jnp.float32
        ).astype(jnp.bfloat16),
        ("context", "dp"),
        scatter_dimension=0,
        tiled=True,
    ).astype(jnp.float32)


def to_owner(slot_rows):
    return lax.all_to_all(slot_rows, "expert", split_axis=0, concat_axis=0, tiled=True)


def to_home(slot_rows):
    return lax.all_to_all(slot_rows, "expert", split_axis=0, concat_axis=0, tiled=True)


def pair_gates(logits, routes, live, experts):
    picked = (routes[:, :, None] == jnp.arange(experts, dtype=jnp.int32)[None, None, :]).astype(
        jnp.float32
    )
    chosen = jnp.sum(picked * logits[:, None, :], axis=-1)
    highest = jnp.max(chosen, axis=-1, keepdims=True)
    exponent = jnp.exp(chosen - highest)
    return (exponent / jnp.sum(exponent, axis=-1, keepdims=True) * live[:, None], picked)


def logit_grad(shares, picked, pair_grad):
    mean_grad = jnp.sum(shares * pair_grad, axis=-1, keepdims=True)
    return jnp.sum((shares * (pair_grad - mean_grad))[:, :, None] * picked, axis=1)


def route_table(routes, live_int, experts, capacity):
    owners = (routes[:, :, None] == jnp.arange(experts, dtype=jnp.int32)[None, None, :]).astype(
        jnp.int32
    )
    owners = owners * live_int[:, None, None]
    used_slots = jnp.sum(owners, axis=1)
    before = jnp.cumsum(used_slots, axis=0) - used_slots
    slot_rank = jnp.sum(before[:, None, :] * owners, axis=-1)
    target = routes * capacity + slot_rank
    slot_hits = (
        target[:, :, None] == jnp.arange(experts * capacity, dtype=jnp.int32)[None, None, :]
    ).astype(jnp.int32)
    return slot_hits * live_int[:, None, None]


def dispatch(table_low, token_rows, experts, capacity):
    sent = jnp.einsum("tkr,td->rd", table_low, token_rows, preferred_element_type=jnp.float32)
    return sent.astype(jnp.bfloat16).reshape(experts, capacity, token_rows.shape[1])


def collect_pairs(table_low, received):
    flat = received.reshape(-1, received.shape[-1])
    return jnp.einsum("tkr,rd->tkd", table_low, flat, preferred_element_type=jnp.float32)


def collect_sum(table_low, received):
    flat = received.reshape(-1, received.shape[-1])
    return jnp.einsum("tkr,rd->td", table_low, flat, preferred_element_type=jnp.float32)


def spread_back(table_int, shares, gradient, experts, capacity):
    weighted = shares[:, :, None] * gradient[:, None, :]
    sent = jnp.einsum("tkr,tkd->rd", table_int.astype(jnp.float32), weighted, precision=PRECISE)
    return sent.astype(jnp.bfloat16).reshape(experts, capacity, gradient.shape[1])


def masked_scores(query_heads, key_heads, query_pos, key_pos):
    scores = jnp.einsum(
        "rhd,khd->hrk", query_heads, key_heads, preferred_element_type=jnp.float32
    ) * HEAD_DIM ** (-0.5)
    return (scores, key_pos[None, None, :] <= query_pos[None, :, None])


def key_scan(shard_piece, block_step, carried):
    piece_len = shard_piece.shape[0]
    block_len = math.gcd(piece_len, 512)
    blocks = shard_piece.reshape(piece_len // block_len, block_len, shard_piece.shape[1])
    firsts = jnp.arange(piece_len // block_len, dtype=jnp.int32) * block_len

    def key_one_block(carry_in, element):
        block_rows, first_key = element
        key_heads = block_rows[:, :QD].reshape(block_len, HEADS, HEAD_DIM)
        value_heads = block_rows[:, QD:].reshape(block_len, HEADS, HEAD_DIM)
        key_pos = first_key + jnp.arange(block_len, dtype=jnp.int32)
        return (block_step(carry_in, key_heads, value_heads, key_pos), None)

    carried, _ = lax.scan(key_one_block, carried, (blocks, firsts))
    return carried


def key_fold(kv_rows, block_step, zeros_init):
    return key_scan(
        lax.all_gather(kv_rows, ("expert", "context"), axis=0, tiled=True), block_step, zeros_init
    )


def gathered_weights(
    layer_input,
    output_grad,
    lengths,
    attn_routes,
    ffn_routes,
    norm1_gain,
    norm2_gain,
    attn_router,
    ffn_router,
    w_kv,
    w_query,
    w_out,
    w_in,
    w_down,
):
    tokens = layer_input.shape[1]
    width = layer_input.shape[2]
    experts = lax.axis_size("expert")
    capacity = tokens * TOP // experts + tokens // 32
    row_count = experts * capacity
    position = lax.axis_index(("expert", "context")) * tokens + jnp.arange(tokens, dtype=jnp.int32)
    live_int = (position < lengths[0]).astype(jnp.int32)
    live = live_int.astype(jnp.float32)
    x_float = layer_input[0].astype(jnp.float32)
    scale_one = rms_scale(x_float)
    normed_one = (x_float * scale_one * norm1_gain).astype(jnp.bfloat16)
    kv_rows = weight_fold(normed_one, w_kv).astype(jnp.bfloat16)
    shares_a, picked_a = pair_gates(
        jnp.dot(normed_one, attn_router, preferred_element_type=jnp.float32),
        attn_routes[0],
        live,
        experts,
    )
    table_a = route_table(attn_routes[0], live_int, experts, capacity)
    low_table_a = table_a.astype(jnp.bfloat16)
    send_rows = dispatch(low_table_a, normed_one, experts, capacity)
    send_pos = jnp.einsum("tkr,t->r", table_a, position).reshape(experts, capacity)
    got_rows, got_pos = (
        lax.all_to_all(send_rows, "expert", split_axis=0, concat_axis=0, tiled=True),
        lax.all_to_all(send_pos, "expert", split_axis=0, concat_axis=0, tiled=True),
    )
    routed_one = got_rows.reshape(row_count, width)
    slot_pos = got_pos.reshape(row_count)
    query = weight_fold(routed_one, w_query[0]).astype(jnp.bfloat16)
    query_heads = query.reshape(row_count, HEADS, HEAD_DIM)

    def stat_step(carry_in, key_heads, value_heads, key_pos):
        highest, running = carry_in
        scores, allowed = masked_scores(query_heads, key_heads, slot_pos, key_pos)
        new_high = jnp.maximum(highest, jnp.max(jnp.where(allowed, scores, -1e30), axis=-1))
        running = running * jnp.exp(highest - new_high) + jnp.sum(
            jnp.where(allowed, jnp.exp(scores - new_high[:, :, None]), 0.0), axis=-1
        )
        return (new_high, running)

    highest, running = key_fold(
        kv_rows,
        stat_step,
        (
            jnp.full((HEADS, row_count), -1e30, jnp.float32),
            jnp.zeros((HEADS, row_count), jnp.float32),
        ),
    )
    log_norm = highest + jnp.log(running)

    def value_step(carry_in, key_heads, value_heads, key_pos):
        scores, allowed = masked_scores(query_heads, key_heads, slot_pos, key_pos)
        probabilities = jnp.where(allowed, jnp.exp(scores - log_norm[:, :, None]), 0.0).astype(
            jnp.bfloat16
        )
        return carry_in + jnp.einsum(
            "hrk,khd->rhd", probabilities, value_heads, preferred_element_type=jnp.float32
        )

    attended = key_fold(kv_rows, value_step, jnp.zeros((row_count, HEADS, HEAD_DIM), jnp.float32))
    attended = attended.reshape(row_count, QD).astype(jnp.bfloat16)
    branch_rows = weight_fold(attended, w_out[0]).astype(jnp.bfloat16)
    branch_back = to_home(branch_rows.reshape(experts, capacity, width))
    branch_pairs = collect_pairs(low_table_a, branch_back)
    residual_one = x_float + jnp.sum(shares_a[:, :, None] * branch_pairs, axis=1)
    scale_two = rms_scale(residual_one)
    normed_two = (residual_one * scale_two * norm2_gain).astype(jnp.bfloat16)
    shares_f, picked_f = pair_gates(
        jnp.dot(normed_two, ffn_router, preferred_element_type=jnp.float32),
        ffn_routes[0],
        live,
        experts,
    )
    table_f = route_table(ffn_routes[0], live_int, experts, capacity)
    low_table_f = table_f.astype(jnp.bfloat16)
    routed_two = to_owner(dispatch(low_table_f, normed_two, experts, capacity)).reshape(
        row_count, width
    )
    both = unit_forward(routed_two, w_in[0])
    hidden = (jax.nn.silu(both[:, :FF]) * both[:, FF:]).astype(jnp.bfloat16)
    down_rows = weight_fold(hidden, w_down[0]).astype(jnp.bfloat16)
    down_back = to_home(down_rows.reshape(experts, capacity, width))
    down_pairs = collect_pairs(low_table_f, down_back)
    mixed = jnp.sum(shares_f[:, :, None] * down_pairs, axis=1)
    layer_output = (live[:, None] * (residual_one + mixed)).astype(jnp.bfloat16)
    grad_out = output_grad[0].astype(jnp.float32) * live[:, None]
    pair_grad_f = jnp.sum(grad_out[:, None, :] * down_pairs, axis=-1)
    d_down = to_owner(spread_back(table_f, shares_f, grad_out, experts, capacity)).reshape(
        row_count, width
    )
    d_hidden = weight_back(d_down, w_down[0])
    gate_part = both[:, :FF]
    up_part = both[:, FF:]
    sigmoid_gate = jax.nn.sigmoid(gate_part)
    d_gate = d_hidden * up_part * sigmoid_gate * (1.0 + gate_part * (1.0 - sigmoid_gate))
    d_up = d_hidden * gate_part * sigmoid_gate
    d_gate_up = jnp.concatenate([d_gate, d_up], axis=1).astype(jnp.bfloat16)
    d_routed_two = unit_backward(d_gate_up, w_in[0]).astype(jnp.bfloat16)
    grad_w_in = unit_grad(d_gate_up, routed_two)
    grad_w_down = weight_grad(hidden, d_down)
    d_copy_two = to_home(d_routed_two.reshape(experts, capacity, width))
    dlog_f = logit_grad(shares_f, picked_f, pair_grad_f)
    d_normed_two = collect_sum(low_table_f, d_copy_two) + jnp.dot(
        dlog_f, ffn_router.astype(jnp.float32).T, precision=PRECISE
    )
    local_ffn_router = jnp.dot(normed_two.astype(jnp.float32).T, dlog_f, precision=PRECISE)
    d_mid, local_gain_two = norm_back(residual_one, scale_two, norm2_gain, d_normed_two)
    d_residual = grad_out + d_mid
    pair_grad_a = jnp.sum(d_residual[:, None, :] * branch_pairs, axis=-1)
    d_branch = to_owner(spread_back(table_a, shares_a, d_residual, experts, capacity)).reshape(
        row_count, width
    )
    d_attended = weight_back(d_branch, w_out[0]).astype(jnp.bfloat16)
    grad_w_out = weight_grad(attended, d_branch)
    delta_rows = jnp.sum(
        (d_attended.astype(jnp.float32) * attended.astype(jnp.float32)).reshape(
            row_count, HEADS, HEAD_DIM
        ),
        axis=-1,
    )
    delta_sum = delta_rows.T
    d_attended_heads = d_attended.reshape(row_count, HEADS, HEAD_DIM)

    def query_grad_step(carry_in, key_heads, value_heads, key_pos):
        scores, allowed = masked_scores(query_heads, key_heads, slot_pos, key_pos)
        probabilities = jnp.where(allowed, jnp.exp(scores - log_norm[:, :, None]), 0.0)
        d_prob = jnp.einsum(
            "rhd,khd->hrk", d_attended_heads, value_heads, preferred_element_type=jnp.float32
        )
        d_scores = (probabilities * (d_prob - delta_sum[:, :, None])).astype(jnp.bfloat16)
        return carry_in + jnp.einsum(
            "hrk,khd->rhd", d_scores, key_heads, preferred_element_type=jnp.float32
        )

    d_query_sum = key_fold(
        kv_rows, query_grad_step, jnp.zeros((row_count, HEADS, HEAD_DIM), jnp.float32)
    )
    d_query = (d_query_sum * HEAD_DIM ** (-0.5)).reshape(row_count, QD).astype(jnp.bfloat16)
    d_routed_one = weight_back(d_query, w_query[0]).astype(jnp.bfloat16)
    grad_w_query = weight_grad(routed_one, d_query)
    d_copy_one = to_home(d_routed_one.reshape(experts, capacity, width))
    own_keys = kv_rows[:, :QD].reshape(tokens, HEADS, HEAD_DIM)
    own_values = kv_rows[:, QD:].reshape(tokens, HEADS, HEAD_DIM)
    zeros_heads = jnp.zeros((tokens, HEADS, HEAD_DIM), jnp.float32)
    carried = (zeros_heads, zeros_heads)
    shard_piece = (
        lax.all_gather(query, ("expert", "context"), axis=0, tiled=True),
        lax.all_gather(d_attended, ("expert", "context"), axis=0, tiled=True),
        lax.all_gather(
            log_norm.T.astype(jnp.bfloat16), ("expert", "context"), axis=0, tiled=True
        ).astype(jnp.float32),
        lax.all_gather(
            delta_rows.astype(jnp.bfloat16), ("expert", "context"), axis=0, tiled=True
        ).astype(jnp.float32),
        lax.all_gather(slot_pos, ("expert", "context"), axis=0, tiled=True),
    )
    piece_len = shard_piece[0].shape[0]
    block_len = math.gcd(piece_len, row_count)

    def body_one_block(carry_in, element):
        query_part, grad_part, norm_part, delta_part, pos_part = element
        query_low = query_part.reshape(block_len, HEADS, HEAD_DIM)
        grad_low = grad_part.reshape(block_len, HEADS, HEAD_DIM)
        scores, allowed = masked_scores(query_low, own_keys, pos_part, position)
        probabilities = jnp.where(allowed, jnp.exp(scores - norm_part.T[:, :, None]), 0.0)
        d_prob = jnp.einsum(
            "rhd,khd->hrk", grad_low, own_values, preferred_element_type=jnp.float32
        )
        d_scores = (probabilities * (d_prob - delta_part.T[:, :, None])).astype(jnp.bfloat16)
        d_keys, d_values = carry_in
        d_keys = d_keys + jnp.einsum(
            "hrk,rhd->khd", d_scores, query_low, preferred_element_type=jnp.float32
        )
        d_values = d_values + jnp.einsum(
            "hrk,rhd->khd",
            probabilities.astype(jnp.bfloat16),
            grad_low,
            preferred_element_type=jnp.float32,
        )
        return ((d_keys, d_values), None)

    shaped = tuple(
        (
            member.reshape((piece_len // block_len, block_len) + member.shape[1:])
            for member in shard_piece
        )
    )
    carried, _ = lax.scan(body_one_block, carried, shaped)
    d_keys, d_values = carried
    d_kv = jnp.concatenate(
        [d_keys.reshape(tokens, QD) * HEAD_DIM ** (-0.5), d_values.reshape(tokens, QD)], axis=1
    ).astype(jnp.bfloat16)
    grad_w_kv = lax.psum(weight_grad(normed_one, d_kv).astype(jnp.bfloat16), "expert").astype(
        jnp.float32
    )
    dlog_a = logit_grad(shares_a, picked_a, pair_grad_a)
    d_normed_one = (
        collect_sum(low_table_a, d_copy_one)
        + weight_back(d_kv, w_kv)
        + jnp.dot(dlog_a, attn_router.astype(jnp.float32).T, precision=PRECISE)
    )
    local_attn_router = jnp.dot(normed_one.astype(jnp.float32).T, dlog_a, precision=PRECISE)
    d_first, local_gain_one = norm_back(x_float, scale_one, norm1_gain, d_normed_one)
    input_grad = d_residual + d_first
    gain_one_sum, gain_two_sum, router_a_sum, router_f_sum = lax.psum(
        (local_gain_one, local_gain_two, local_attn_router, local_ffn_router),
        ("expert", "context", "dp"),
    )
    return (
        layer_output[None],
        input_grad[None],
        gain_one_sum,
        gain_two_sum,
        router_a_sum,
        router_f_sum,
        grad_w_kv,
        grad_w_query[None],
        grad_w_out[None],
        grad_w_in[None],
        grad_w_down[None],
    )


MESH = pl.DeviceIdType.MESH
SHARE = ("context", "dp")


class Place:
    def __init__(self):
        self.e = lax.axis_index("expert")
        self.x = lax.axis_index("context")
        self.z = lax.axis_index("dp")
        self.own = (self.e, self.x)
        self.c = lax.rem(self.e, 2)
        self.sib = (self.e + 1 - 2 * self.c, self.x)
        self.across = (lax.rem(self.e + 2, 4), self.x)
        self.share = self.x * 4 + self.z
        self.cols = self.columns(self.e, self.x, self.c)
        self.sib_cols = self.columns(self.sib[0], self.x, 1 - self.c)

    def columns(self, e, x, c):
        first = (lax.rem(e + 2 * c, 4), lax.rem(x + 1 - c, 2))
        second = (lax.rem(e + 2 * (1 - c), 4), lax.rem(x + c, 2))
        return ((e, x), first, second, (lax.rem(e + 2, 4), 1 - x))

    def dev(self, col, z=None):
        return (col[0], col[1], self.z if z is None else z)

    def mate(self, d):
        share = lax.rem(self.share + d, 8)
        return (self.e, lax.div(share, 4), lax.rem(share, 4))

    def block(self, col, z):
        return z * 8 + col[0] * 2 + col[1]


def signal(barrier, dev):
    pl.semaphore_signal(barrier, inc=1, device_id=dev, device_id_type=MESH)


def greet(pc):
    barrier = pltpu.get_barrier_semaphore()
    for col in (pc.sib, pc.cols[1], pc.cols[2]):
        signal(barrier, pc.dev(col))
    pl.when(pc.z > 0)(lambda: signal(barrier, pc.dev(pc.own, pc.z - 1)))
    pl.when(pc.z < 3)(lambda: signal(barrier, pc.dev(pc.own, pc.z + 1)))
    pl.semaphore_wait(barrier, 3 + lax.div(pc.z + 3, 4) + lax.div(6 - pc.z, 4))


class Copies:
    def __init__(self, parts):
        self.parts = parts

    def start(self):
        for part in self.parts:
            part.start()

    def wait_send(self):
        for part in self.parts:
            part.wait_send()

    def wait_recv(self):
        for part in self.parts:
            part.wait_recv()


def remote(src, dst, send, recv, dev):
    return pltpu.make_async_remote_copy(
        src_ref=src, dst_ref=dst, send_sem=send, recv_sem=recv, device_id=dev, device_id_type=MESH
    )


def when_in(cond, run):
    if cond is True:
        run()
    else:
        pl.when(cond)(run)


class Gather:
    sems = ((), (2, 4), (2, 4), (7,), (7,), (2, 7), (2, 7), (4, 7), (4, 7))

    def __init__(self, pc, ins, outs, sems):
        self.pc, self.ins, self.outs = pc, ins, outs
        self.loc, self.zs, self.zr, self.fs, self.fr, self.ss, self.sr, self.bs, self.br = sems

    @classmethod
    def scratch(cls, payloads):
        return [pltpu.SemaphoreType.DMA((payloads,) + shape) for shape in cls.sems]

    def copies(self, src_own, blk, send, recv, at, dev):
        return Copies(
            [
                remote(
                    self.ins[p] if src_own else self.outs[p].at[blk],
                    self.outs[p].at[blk],
                    send.at[(p,) + at],
                    recv.at[(p,) + at],
                    dev,
                )
                for p in range(len(self.ins))
            ]
        )

    def hop(self, col, d, kind):
        pc = self.pc
        blk = pc.block(pc.cols[col], pc.z + d)
        own = col == 0 and d == 0
        if kind == "f":
            return self.copies(own, blk, self.fs, self.fr, (d + 3,), pc.dev(pc.cols[1]))
        if kind == "s":
            return self.copies(own, blk, self.ss, self.sr, (col, d + 3), pc.dev(pc.cols[2]))
        return self.copies(own, blk, self.bs, self.br, (col, d + 3), pc.dev(pc.sib))

    def line(self, d, up):
        pc = self.pc
        dev = pc.dev(pc.own, pc.z + 1 if up else pc.z - 1)
        blk = pc.block(pc.own, pc.z + d)
        return self.copies(d == 0, blk, self.zs, self.zr, (0 if up else 1, abs(d)), dev)

    def arrival(self, col, d, recv, at, dev):
        blk = self.pc.block(col, self.pc.z + d)
        return self.copies(False, blk, recv, recv, at, dev)

    def present(self, d):
        return True if d == 0 else (self.pc.z + d >= 0) & (self.pc.z + d <= 3)

    def keep_own(self):
        pc = self.pc
        return [
            pltpu.make_async_copy(
                self.ins[p], self.outs[p].at[pc.block(pc.own, pc.z)], self.loc.at[p]
            )
            for p in range(len(self.ins))
        ]

    def start(self):
        for copy in self.keep_own():
            copy.start()

    def own_line(self, d):
        pc = self.pc

        def run():
            if d < 0:
                below = pc.dev(pc.own, pc.z - 1)
                self.arrival(pc.own, d, self.zr, (0, -d - 1), below).wait_recv()
            if d > 0:
                above = pc.dev(pc.own, pc.z + 1)
                self.arrival(pc.own, d, self.zr, (1, d - 1), above).wait_recv()
            if d <= 0:
                pl.when(pc.z < 3)(lambda: self.line(d, True).start())
            if d >= 0:
                pl.when(pc.z > 0)(lambda: self.line(d, False).start())
            for kind in ("f", "s", "b"):
                self.hop(0, d, kind).start()

        when_in(self.present(d), run)

    def first_col(self, d):
        pc = self.pc

        def run():
            self.arrival(pc.cols[1], d, self.fr, (d + 3,), pc.dev(pc.cols[1])).wait_recv()
            self.hop(1, d, "s").start()
            self.hop(1, d, "b").start()

        when_in(self.present(d), run)

    def last_cols(self, d):
        pc = self.pc

        def run():
            for col, sent in ((2, 0), (3, 1)):
                dev = pc.dev(pc.cols[2])
                self.arrival(pc.cols[col], d, self.sr, (sent, d + 3), dev).wait_recv()
                self.hop(col, d, "b").start()

        when_in(self.present(d), run)

    def finish(self, d):
        pc = self.pc

        def run():
            for col in range(4):
                dev = pc.dev(pc.sib)
                self.arrival(pc.sib_cols[col], d, self.br, (col, d + 3), dev).wait_recv()
            self.hop(0, d, "f").wait_send()
            for col in (0, 1):
                self.hop(col, d, "s").wait_send()
            for col in range(4):
                self.hop(col, d, "b").wait_send()
            if d <= 0:
                pl.when(pc.z < 3)(lambda: self.line(d, True).wait_send())
            if d >= 0:
                pl.when(pc.z > 0)(lambda: self.line(d, False).wait_send())

        when_in(self.present(d), run)

    def end(self):
        for copy in self.keep_own():
            copy.wait()

    def events(self):
        steps = [(self.own_line, 0)]
        for s in (1, 2, 3):
            steps += [(self.own_line, -s), (self.own_line, s)]
            steps += [(self.first_col, d) for d in sorted({1 - s, s - 1})]
        steps += [(self.first_col, -3), (self.first_col, 3)]
        order = (0, -1, 1, -2, 2, -3, 3)
        steps += [(self.last_cols, d) for d in order] + [(self.finish, d) for d in order]
        return [lambda run=run, d=d: run(d) for run, d in steps]


def gather_kernel(count, *refs):
    pc = Place()
    gather = Gather(pc, refs[:count], refs[count : 2 * count], refs[2 * count :])
    gather.start()
    greet(pc)
    for event in gather.events():
        event()
    gather.end()


def gather_all(blocks, cid):
    count = len(blocks)
    return pl.pallas_call(
        functools.partial(gather_kernel, count),
        out_shape=[jax.ShapeDtypeStruct((32,) + b.shape, b.dtype) for b in blocks],
        in_specs=[pl.BlockSpec(memory_space=pltpu.VMEM)] * count,
        out_specs=[pl.BlockSpec(memory_space=pl.ANY)] * count,
        scratch_shapes=Gather.scratch(count),
        compiler_params=pltpu.CompilerParams(collective_id=cid, has_side_effects=True),
        name="gather_all",
    )(*blocks)


class Scatter:
    sems = ((4, 4), (4, 4), (4, 4), (4, 2), (4, 2), (4,), (4,), (2, 4), (2, 4))

    def __init__(self, pc, ins, bufs, sems):
        self.pc, self.ins = pc, ins
        count = len(ins)
        self.acc, self.sib, self.sec, self.fst, self.zin = (
            bufs[i * count : (i + 1) * count] for i in range(5)
        )
        self.ld, self.bs, self.br, self.ss, self.sr, self.fs, self.fr, self.zs, self.zr = sems
        inner = lax.rem(lax.div(pc.z + 1, 2), 2)
        low = 1 - lax.div(pc.z, 2)

        def group(k):
            v = (1 - inner) * k + inner * (0, 1, 3, 2)[k]
            return low * (3 - v) + (1 - low) * v

        self.group = group

    @classmethod
    def scratch(cls, blocks):
        bufs = []
        for lead in ((4, 4), (4, 4), (4, 2), (4,), (2, 4)):
            bufs += [pltpu.VMEM(lead + shape, dtype) for shape, dtype in blocks]
        return bufs + [pltpu.SemaphoreType.DMA((len(blocks),) + s) for s in cls.sems]

    def copies(self, src, dst, send, recv, sent_at, got_at, dev):
        return Copies(
            [
                remote(src(p), dst(p), send.at[(p,) + sent_at], recv.at[(p,) + got_at], dev)
                for p in range(len(self.ins))
            ]
        )

    def loads(self, k, col):
        pc = self.pc
        blk = pc.block(pc.cols[col], self.group(k))
        return [
            pltpu.make_async_copy(self.ins[p].at[blk], self.acc[p].at[k, col], self.ld.at[p, k, col])
            for p in range(len(self.ins))
        ]

    def to_sib(self, k, col):
        pc = self.pc
        blk = pc.block(pc.sib_cols[col], self.group(k))
        return self.copies(
            lambda p: self.ins[p].at[blk], lambda p: self.sib[p].at[k, col],
            self.bs, self.br, (k, col), (k, col), pc.dev(pc.sib),
        )

    def to_second(self, k, j):
        pc = self.pc
        return self.copies(
            lambda p: self.acc[p].at[k, 2 + j], lambda p: self.sec[p].at[k, j],
            self.ss, self.sr, (k, j), (k, j), pc.dev(pc.cols[2]),
        )

    def to_first(self, k):
        pc = self.pc
        return self.copies(
            lambda p: self.acc[p].at[k, 1], lambda p: self.fst[p].at[k],
            self.fs, self.fr, (k,), (k,), pc.dev(pc.cols[1]),
        )

    def to_z(self, k, up):
        pc, g, i = self.pc, self.group(k), 0 if up else 1
        return self.copies(
            lambda p: self.acc[p].at[k, 0], lambda p: self.zin[p].at[i, g],
            self.zs, self.zr, (i, k), (i, g), pc.dev(pc.own, pc.z + 1 if up else pc.z - 1),
        )

    def from_z(self, g, i):
        pc = self.pc
        return self.copies(
            lambda p: self.acc[p].at[0, 0], lambda p: self.zin[p].at[i, g],
            self.zs, self.zr, (i, 0), (i, g), pc.dev(pc.own, pc.z - 1 if i == 0 else pc.z + 1),
        )

    def add(self, k, col, others):
        for acc, other in zip(self.acc, others):
            rows, step = acc.shape[2], min(16, acc.shape[2])

            def body(i, carry, acc=acc, other=other, step=step):
                r = pl.ds(pl.multiple_of(i * step, step), step)
                both = acc[k, col, r, :].astype(jnp.float32) + other[r, :].astype(jnp.float32)
                acc[k, col, r, :] = both.astype(acc.dtype)
                return carry

            lax.fori_loop(0, rows // step, body, 0)

    def start_loads(self):
        for k in range(4):
            for col in (2, 3, 1, 0):
                for copy in self.loads(k, col):
                    copy.start()

    def start(self):
        for k in range(4):
            for col in (2, 3, 1, 0):
                self.to_sib(k, col).start()

    def join(self, k, col):
        for copy in self.loads(k, col):
            copy.wait()
        self.to_sib(k, col).wait_recv()
        self.add(k, col, [buf.at[k, col] for buf in self.sib])

    def stage_a(self, k):
        for j in (0, 1):
            self.join(k, 2 + j)
            self.to_second(k, j).start()

    def stage_b(self, k):
        self.join(k, 1)
        self.to_second(k, 1).wait_recv()
        self.add(k, 1, [buf.at[k, 1] for buf in self.sec])
        self.to_first(k).start()
        self.join(k, 0)

    def stage_c(self, k):
        z = self.pc.z
        self.to_second(k, 0).wait_recv()
        self.add(k, 0, [buf.at[k, 0] for buf in self.sec])
        self.to_first(k).wait_recv()
        self.add(k, 0, [buf.at[k] for buf in self.fst])
        g = self.group(k)

        def arrive(i):
            self.from_z(g, i).wait_recv()
            self.add(k, 0, [buf.at[i, g] for buf in self.zin])

        def upward():
            pl.when(z > 0)(lambda: arrive(0))
            self.to_z(k, True).start()

        def downward():
            pl.when(z < 3)(lambda: arrive(1))
            self.to_z(k, False).start()

        if k < 3:
            pl.when(g > z)(upward)
            pl.when(g < z)(downward)
        else:
            pl.when(z > 0)(lambda: arrive(0))
            pl.when(z < 3)(lambda: arrive(1))

    def events(self):
        a, b, c = self.stage_a, self.stage_b, self.stage_c
        steps = [(a, 0), (a, 1), (b, 0), (a, 2), (b, 1), (c, 0), (a, 3), (b, 2), (c, 1), (b, 3)]
        return [lambda run=run, k=k: run(k) for run, k in steps + [(c, 2), (c, 3)]]

    def end(self):
        z = self.pc.z
        for k in range(4):
            for col in range(4):
                self.to_sib(k, col).wait_send()
            for j in (0, 1):
                self.to_second(k, j).wait_send()
            self.to_first(k).wait_send()
            if k < 3:
                pl.when(self.group(k) > z)(lambda: self.to_z(k, True).wait_send())
                pl.when(self.group(k) < z)(lambda: self.to_z(k, False).wait_send())


def scatter_kernel(count, *refs):
    pc = Place()
    outs = refs[count : 2 * count]
    scatter = Scatter(pc, refs[:count], refs[2 * count : 7 * count], refs[7 * count :])
    scatter.start_loads()
    greet(pc)
    scatter.start()
    for event in scatter.events():
        event()
    for p in range(count):
        outs[p][...] = scatter.acc[p][3, 0]
    scatter.end()


def scatter_all(wholes, cid):
    count = len(wholes)
    blocks = [(w.shape[1:], w.dtype) for w in wholes]
    return pl.pallas_call(
        functools.partial(scatter_kernel, count),
        out_shape=[jax.ShapeDtypeStruct(*b) for b in blocks],
        in_specs=[pl.BlockSpec(memory_space=pl.ANY)] * count,
        out_specs=[pl.BlockSpec(memory_space=pltpu.VMEM)] * count,
        scratch_shapes=Scatter.scratch(blocks),
        compiler_params=pltpu.CompilerParams(
            collective_id=cid, has_side_effects=True, vmem_limit_bytes=48 << 20
        ),
        name="scatter_all",
    )(*wholes)


def sum_kernel(v_ref, out_ref, cur, got, lines, send, recv, zsend, zrecv):
    pc = Place()
    z = pc.z
    near = (pc.sib, (pc.e, 1 - pc.x), (lax.rem(pc.e + 2, 4), pc.x))
    barrier = pltpu.get_barrier_semaphore()
    for col in near:
        signal(barrier, pc.dev(col))
    for d in (1, 2, 3):
        signal(barrier, pc.dev(pc.own, lax.rem(z + d, 4)))
    pl.semaphore_wait(barrier, 6)
    for s, col in enumerate(near):
        src = v_ref if s == 0 else cur.at[s - 1]
        copy = remote(src, got.at[s], send.at[s], recv.at[s], pc.dev(col))
        copy.start()
        copy.wait_recv()
        cur[s] = src[...] + got[s]

    def along(d):
        there = lax.rem(z + d, 4)
        return remote(cur.at[2], lines.at[z], zsend.at[d], zrecv.at[z], pc.dev(pc.own, there))

    for d in (1, 2, 3):
        along(d).start()
    for d in (1, 2, 3):
        source = lax.rem(z + d, 4)
        remote(
            cur.at[2], lines.at[source], zsend.at[0], zrecv.at[source], pc.dev(pc.own, source)
        ).wait_recv()
    lines[z] = cur[2]
    out_ref[...] = ((lines[0] + lines[1]) + lines[2]) + lines[3]
    for s, col in enumerate(near):
        src = v_ref if s == 0 else cur.at[s - 1]
        remote(src, got.at[s], send.at[s], recv.at[s], pc.dev(col)).wait_send()
    for d in (1, 2, 3):
        along(d).wait_send()


def sum_all(v, cid):
    D = pltpu.SemaphoreType.DMA
    return pl.pallas_call(
        sum_kernel,
        out_shape=jax.ShapeDtypeStruct(v.shape, v.dtype),
        in_specs=[pl.BlockSpec(memory_space=pltpu.VMEM)],
        out_specs=pl.BlockSpec(memory_space=pltpu.VMEM),
        scratch_shapes=[
            pltpu.VMEM((3,) + v.shape, v.dtype),
            pltpu.VMEM((3,) + v.shape, v.dtype),
            pltpu.VMEM((4,) + v.shape, v.dtype),
            D((3,)), D((3,)), D((4,)), D((4,)),
        ],
        compiler_params=pltpu.CompilerParams(collective_id=cid, has_side_effects=True),
        name="sum_all",
    )(v)


def greet_share(pc):
    barrier = pltpu.get_barrier_semaphore()
    for d in range(1, 8):
        signal(barrier, pc.mate(d))
    signal(barrier, pc.dev(pc.across))
    signal(barrier, pc.dev(pc.sib))
    pl.semaphore_wait(barrier, 9)


def lanes(start, size):
    return pl.ds(pl.multiple_of(start, size), size)


class ColumnWeights:
    sems = ((2,), (8,), (8,), (8,), (8,), (3,), (3,))

    def __init__(self, pc, query, kv, out, sems):
        self.pc, self.query, self.kv, self.out = pc, query, kv, out
        self.loc, self.qs, self.qr, self.ks, self.kr, self.ms, self.mr = sems

    @classmethod
    def scratch(cls):
        return [pltpu.SemaphoreType.DMA(s) for s in cls.sems]

    def quarter(self, e):
        return lanes(256 + 128 * e, 128)

    def source(self, kind, share):
        e = self.pc.e
        if kind == 0:
            return self.query.at[:, lanes(share * 256, 256)]
        return self.kv.at[:, lanes(lax.div(e, 2) * QD + share * 256 + lax.rem(e, 2) * 128, 128)]

    def place(self, kind, share):
        return self.out.at[share, :, pl.ds(0, 256) if kind == 0 else self.quarter(self.pc.e)]

    def keep(self, kind):
        share = self.pc.share
        return pltpu.make_async_copy(
            self.source(kind, share), self.place(kind, share), self.loc.at[kind]
        )

    def sent(self, kind, d):
        pc = self.pc
        send, recv = ((self.qs, self.qr), (self.ks, self.kr))[kind]
        src = self.source(kind, lax.rem(pc.share + d, 8))
        return remote(src, self.place(kind, pc.share), send.at[d], recv.at[pc.share], pc.mate(d))

    def landed(self, kind, d):
        share = lax.rem(self.pc.share + d, 8)
        send, recv = ((self.qs, self.qr), (self.ks, self.kr))[kind]
        ref = self.place(kind, share)
        return remote(ref, ref, send.at[0], recv.at[share], self.pc.mate(d))

    def passed(self, i):
        pc = self.pc
        e = pc.across[0] if i == 2 else pc.e
        ref = self.out.at[:, :, self.quarter(e)]
        dev = pc.dev(pc.across if i == 0 else pc.sib)
        return remote(ref, ref, self.ms.at[i], self.mr.at[i], dev)

    def came(self, i):
        pc = self.pc
        e = (pc.across[0], pc.sib[0], lax.rem(pc.sib[0] + 2, 4))[i]
        ref = self.out.at[:, :, self.quarter(e)]
        return remote(ref, ref, self.ms.at[i], self.mr.at[i], pc.dev(pc.across if i == 0 else pc.sib))

    def start(self):
        for kind in (1, 0):
            self.keep(kind).start()
            for d in range(1, 8):
                self.sent(kind, d).start()

    def gathered(self):
        self.keep(1).wait()
        for d in range(1, 8):
            self.landed(1, d).wait_recv()
        self.passed(0).start()
        self.passed(1).start()

    def crossed(self):
        self.came(0).wait_recv()
        self.passed(2).start()

    def finish(self):
        self.keep(0).wait()
        for d in range(1, 8):
            self.landed(0, d).wait_recv()
            for kind in (0, 1):
                self.sent(kind, d).wait_send()
        for i in (1, 2):
            self.came(i).wait_recv()
        for i in range(3):
            self.passed(i).wait_send()


class ColumnGrads:
    sems = ((3,), (8,), (8,), (2,), (2,), (8,), (8,), (4, 8), (4, 8), (1,))

    def __init__(self, pc, grad, query, kv, bufs, sems):
        self.pc, self.grad, self.query, self.kv = pc, grad, query, kv
        self.own, self.other, self.sib, self.across = bufs
        (self.ld, self.qs, self.qr, self.bs, self.br, self.ks, self.kr, self.ms, self.mr, self.loc) = sems

    @classmethod
    def scratch(cls):
        part = lambda *lead: pltpu.VMEM(lead + (8, 256, 128), jnp.bfloat16)
        bufs = [part(), part(), part(2), part()]
        return bufs + [pltpu.SemaphoreType.DMA(s) for s in cls.sems]

    def quarter(self, e):
        return self.grad.at[:, :, lanes(256 + 128 * e, 128)]

    def load(self, i):
        pc = self.pc
        e, to = ((pc.e, self.own), (pc.across[0], self.other))[i]
        return pltpu.make_async_copy(self.quarter(e), to, self.ld.at[i])

    def place(self, e, share):
        start = lax.div(e, 2) * QD + share * 256 + lax.rem(e, 2) * 128
        return self.kv.at[:, lanes(start, 128)]

    def row_copies(self, e, i, dev):
        return Copies(
            [
                remote(
                    self.place(e, share), self.place(e, share),
                    self.ms.at[i, share], self.mr.at[i, share], dev,
                )
                for share in range(8)
            ]
        )

    def keep_query(self):
        pc = self.pc
        return pltpu.make_async_copy(
            self.grad.at[pc.share, :, pl.ds(0, 256)],
            self.query.at[:, lanes(pc.share * 256, 256)],
            self.ld.at[2],
        )

    def query_to(self, d):
        pc = self.pc
        return remote(
            self.grad.at[lax.rem(pc.share + d, 8), :, pl.ds(0, 256)],
            self.query.at[:, lanes(pc.share * 256, 256)],
            self.qs.at[d], self.qr.at[pc.share], pc.mate(d),
        )

    def query_from(self, d):
        pc = self.pc
        share = lax.rem(pc.share + d, 8)
        ref = self.query.at[:, lanes(share * 256, 256)]
        return remote(ref, ref, self.qs.at[0], self.qr.at[share], pc.mate(d))

    def to_sib(self, i):
        pc = self.pc
        e = pc.sib[0] if i == 0 else lax.rem(pc.sib[0] + 2, 4)
        return remote(self.quarter(e), self.sib.at[i], self.bs.at[i], self.br.at[i], pc.dev(pc.sib))

    def pass_on(self, i):
        pc = self.pc
        dev = pc.dev(pc.across if i < 2 else pc.sib)
        if i == 0:
            return remote(self.other, self.across, self.ms.at[0, 0], self.mr.at[0, 0], dev)
        return self.row_copies(pc.across[0] if i == 3 else pc.e, i, dev)

    def came(self, i):
        pc = self.pc
        e = (pc.across[0], pc.sib[0], lax.rem(pc.sib[0] + 2, 4))[i - 1]
        return self.row_copies(e, i, pc.dev(pc.across if i < 2 else pc.sib))

    def keep_kv(self):
        pc = self.pc
        return pltpu.make_async_copy(
            self.own.at[pc.share], self.place(pc.e, pc.share), self.loc.at[0]
        )

    def kv_to(self, d):
        pc = self.pc
        return remote(
            self.own.at[lax.rem(pc.share + d, 8)], self.place(pc.e, pc.share),
            self.ks.at[d], self.kr.at[pc.share], pc.mate(d),
        )

    def kv_from(self, d):
        pc = self.pc
        share = lax.rem(pc.share + d, 8)
        ref = self.place(pc.e, share)
        return remote(ref, ref, self.ks.at[0], self.kr.at[share], pc.mate(d))

    def add(self, ref, other):
        def body(i, carry):
            share, r = lax.div(i, 16), pl.ds(pl.multiple_of(lax.rem(i, 16) * 16, 16), 16)
            both = ref[share, r, :].astype(jnp.float32) + other[share, r, :].astype(jnp.float32)
            ref[share, r, :] = both.astype(ref.dtype)
            return carry

        lax.fori_loop(0, 128, body, 0)

    def start(self):
        for i in (0, 1):
            self.load(i).start()
        self.keep_query().start()
        for i in (1, 0):
            self.to_sib(i).start()
        for d in range(1, 8):
            self.query_to(d).start()

    def cores(self):
        for i in (0, 1):
            self.load(i).wait()
        self.to_sib(1).wait_recv()
        self.add(self.other, self.sib.at[1])
        self.pass_on(0).start()
        self.to_sib(0).wait_recv()
        self.add(self.own, self.sib.at[0])

    def crossed(self):
        self.pass_on(0).wait_recv()
        self.add(self.own, self.across)
        self.keep_kv().start()
        for d in range(1, 8):
            self.kv_to(d).start()

    def landed(self):
        self.keep_kv().wait()
        for d in range(1, 8):
            self.kv_from(d).wait_recv()
        self.pass_on(1).start()
        self.pass_on(2).start()

    def returned(self):
        self.came(1).wait_recv()
        self.pass_on(3).start()

    def finish(self):
        self.keep_query().wait()
        for i in (2, 3):
            self.came(i).wait_recv()
        for i in (0, 1):
            self.to_sib(i).wait_send()
        for i in range(4):
            self.pass_on(i).wait_send()
        for d in range(1, 8):
            self.query_from(d).wait_recv()
            self.query_to(d).wait_send()
            self.kv_to(d).wait_send()


def insert(events, extra):
    out = []
    for i, event in enumerate(events):
        out += [e for place, e in extra if place == i] + [event]
    return out + [e for place, e in extra if place >= len(events)]


def first_gather_kernel(count, *refs):
    ins, refs = refs[: count + 2], refs[count + 2 :]
    outs, sems = refs[: count + 1], refs[count + 1 :]
    pc = Place()
    cut = len(Gather.sems)
    gather = Gather(pc, ins[:count], outs[:count], sems[:cut])
    weights = ColumnWeights(pc, ins[count], ins[count + 1], outs[count], sems[cut:])
    gather.start()
    greet_share(pc)
    events = gather.events()
    extra = ((1, weights.start), (6, weights.gathered), (12, weights.crossed), (99, weights.finish))
    for event in insert(events, extra):
        event()
    gather.end()


def first_gather(blocks, query, kv, cid):
    count = len(blocks)
    rows = query.shape[0]
    hbm = pl.BlockSpec(memory_space=pl.ANY)
    return pl.pallas_call(
        functools.partial(first_gather_kernel, count),
        out_shape=[jax.ShapeDtypeStruct((32,) + b.shape, b.dtype) for b in blocks]
        + [jax.ShapeDtypeStruct((8, rows, 768), query.dtype)],
        in_specs=[pl.BlockSpec(memory_space=pltpu.VMEM)] * count + [hbm, hbm],
        out_specs=[hbm] * (count + 1),
        scratch_shapes=Gather.scratch(count) + ColumnWeights.scratch(),
        compiler_params=pltpu.CompilerParams(collective_id=cid, has_side_effects=True),
        name="first_gather",
    )(*blocks, query, kv)


def last_scatter_kernel(count, *refs):
    ins, refs = refs[: count + 1], refs[count + 1 :]
    outs, refs = refs[: count + 2], refs[count + 2 :]
    cut = 5 * count + len(Scatter.sems)
    bufs, sems = refs[: 5 * count], refs[5 * count : cut]
    pc = Place()
    scatter = Scatter(pc, ins[:count], bufs, sems)
    grads = ColumnGrads(pc, ins[count], outs[count], outs[count + 1], refs[cut : cut + 4], refs[cut + 4 :])
    scatter.start_loads()
    greet_share(pc)
    scatter.start()
    grads.start()
    extra = (
        (2, grads.cores), (4, grads.crossed), (7, grads.landed), (9, grads.returned), (99, grads.finish),
    )
    for event in insert(scatter.events(), extra):
        event()
    for p in range(count):
        outs[p][...] = scatter.acc[p][3, 0]
    scatter.end()


def last_scatter(wholes, grad, cid):
    count = len(wholes)
    blocks = [(w.shape[1:], w.dtype) for w in wholes]
    rows = grad.shape[1]
    hbm, vmem = pl.BlockSpec(memory_space=pl.ANY), pl.BlockSpec(memory_space=pltpu.VMEM)
    return pl.pallas_call(
        functools.partial(last_scatter_kernel, count),
        out_shape=[jax.ShapeDtypeStruct(*b) for b in blocks]
        + [
            jax.ShapeDtypeStruct((rows, 8 * 256), grad.dtype),
            jax.ShapeDtypeStruct((rows, 2 * QD), grad.dtype),
        ],
        in_specs=[hbm] * (count + 1),
        out_specs=[vmem] * count + [hbm, hbm],
        scratch_shapes=Scatter.scratch(blocks) + ColumnGrads.scratch(),
        compiler_params=pltpu.CompilerParams(
            collective_id=cid, has_side_effects=True, vmem_limit_bytes=52 << 20
        ),
        name="last_scatter",
    )(*wholes, grad)


def attend_kernel(qkv_ref, att_ref, lse_ref):
    length = qkv_ref.shape[0]
    tile = 256
    heads = att_ref.shape[1] // HEAD_DIM
    for head in range(heads):
        at = lambda part: pl.ds((part * heads + head) * HEAD_DIM, HEAD_DIM)
        for first in range(0, length, tile):
            last = first + tile
            q = qkv_ref[pl.ds(first, tile), at(0)]
            k = qkv_ref[pl.ds(0, last), at(1)]
            v = qkv_ref[pl.ds(0, last), at(2)]
            scores = lax.dot_general(
                k, q, (((1,), (1,)), ((), ())), preferred_element_type=jnp.float32
            ) * HEAD_DIM ** (-0.5)
            key_pos = lax.broadcasted_iota(jnp.int32, scores.shape, 0)
            query_pos = first + lax.broadcasted_iota(jnp.int32, scores.shape, 1)
            scores = jnp.where(key_pos <= query_pos, scores, -1e30)
            highest = jnp.max(scores, axis=0, keepdims=True)
            exponent = jnp.exp(scores - highest)
            total = jnp.sum(exponent, axis=0, keepdims=True)
            mixed = lax.dot_general(
                v,
                exponent.astype(jnp.bfloat16),
                (((0,), (0,)), ((), ())),
                preferred_element_type=jnp.float32,
            )
            mixed = mixed * (1.0 / total)
            att_ref[pl.ds(first, tile), pl.ds(head * HEAD_DIM, HEAD_DIM)] = mixed.T.astype(
                jnp.bfloat16
            )
            lse_ref[0, pl.ds(head, 1), pl.ds(first, tile)] = highest + jnp.log(total)


def attend(qkv, slots):
    rows, width = qkv.shape
    length = rows // slots
    out = width // 3
    return pl.pallas_call(
        attend_kernel,
        grid=(slots,),
        out_shape=(
            jax.ShapeDtypeStruct((rows, out), jnp.bfloat16),
            jax.ShapeDtypeStruct((slots, out // HEAD_DIM, length), jnp.float32),
        ),
        in_specs=[pl.BlockSpec((length, width), lambda s: (s, 0))],
        out_specs=(
            pl.BlockSpec((length, out), lambda s: (s, 0)),
            pl.BlockSpec((1, out // HEAD_DIM, length), lambda s: (s, 0, 0)),
        ),
        compiler_params=pltpu.CompilerParams(vmem_limit_bytes=48 << 20),
        name="attend",
    )(qkv)


def attend_back_kernel(qkv_ref, du_ref, lse_ref, gate_ref, dqkv_ref, dgate_ref, dk_acc, dv_acc):
    length = qkv_ref.shape[0]
    tile = 256
    heads = du_ref.shape[1] // HEAD_DIM
    scale = HEAD_DIM ** (-0.5)
    for head in range(heads):
        at = lambda part: pl.ds((part * heads + head) * HEAD_DIM, HEAD_DIM)
        dk_acc[...] = jnp.zeros_like(dk_acc)
        dv_acc[...] = jnp.zeros_like(dv_acc)
        for first in range(0, length, tile):
            last = first + tile
            q = qkv_ref[pl.ds(first, tile), at(0)]
            k = qkv_ref[pl.ds(0, last), at(1)]
            v = qkv_ref[pl.ds(0, last), at(2)]
            du = du_ref[pl.ds(first, tile), pl.ds(head * HEAD_DIM, HEAD_DIM)]
            gate = gate_ref[0, :, pl.ds(first, tile)]
            lse = lse_ref[0, pl.ds(head, 1), pl.ds(first, tile)]
            scores = (
                lax.dot_general(k, q, (((1,), (1,)), ((), ())), preferred_element_type=jnp.float32)
                * scale
            )
            key_pos = lax.broadcasted_iota(jnp.int32, scores.shape, 0)
            query_pos = first + lax.broadcasted_iota(jnp.int32, scores.shape, 1)
            probs = jnp.where(key_pos <= query_pos, jnp.exp(scores - lse), 0.0)
            d_prob = lax.dot_general(
                v, du, (((1,), (1,)), ((), ())), preferred_element_type=jnp.float32
            )
            along = jnp.sum(probs * d_prob, axis=0, keepdims=True)
            dgate_ref[0, pl.ds(head, 1), pl.ds(first, tile)] = along
            shared = probs * gate
            d_scores = (shared * (d_prob - along)).astype(jnp.bfloat16)
            dq = lax.dot_general(
                d_scores, k, (((0,), (0,)), ((), ())), preferred_element_type=jnp.float32
            )
            dqkv_ref[pl.ds(first, tile), at(0)] = (dq * scale).astype(jnp.bfloat16)
            dk_acc[pl.ds(0, last), :] += jnp.dot(d_scores, q, preferred_element_type=jnp.float32)
            dv_acc[pl.ds(0, last), :] += jnp.dot(
                shared.astype(jnp.bfloat16), du, preferred_element_type=jnp.float32
            )
        dqkv_ref[:, at(1)] = (dk_acc[...] * scale).astype(jnp.bfloat16)
        dqkv_ref[:, at(2)] = dv_acc[...].astype(jnp.bfloat16)


def attend_back(qkv, du, lse, gate, slots):
    rows, width = qkv.shape
    length = rows // slots
    out = width // 3
    heads = out // HEAD_DIM
    return pl.pallas_call(
        attend_back_kernel,
        grid=(slots,),
        out_shape=(
            jax.ShapeDtypeStruct((rows, width), jnp.bfloat16),
            jax.ShapeDtypeStruct((slots, heads, length), jnp.float32),
        ),
        in_specs=[
            pl.BlockSpec((length, width), lambda s: (s, 0)),
            pl.BlockSpec((length, out), lambda s: (s, 0)),
            pl.BlockSpec((1, heads, length), lambda s: (s, 0, 0)),
            pl.BlockSpec((1, 1, length), lambda s: (s, 0, 0)),
        ],
        out_specs=(
            pl.BlockSpec((length, width), lambda s: (s, 0)),
            pl.BlockSpec((1, heads, length), lambda s: (s, 0, 0)),
        ),
        scratch_shapes=[
            pltpu.VMEM((length, HEAD_DIM), jnp.float32),
            pltpu.VMEM((length, HEAD_DIM), jnp.float32),
        ],
        compiler_params=pltpu.CompilerParams(vmem_limit_bytes=48 << 20),
        name="attend_back",
    )(qkv, du, lse, gate)


def as_rows(*columns):
    rows = jnp.concatenate([c.T for c in columns], axis=0)
    return jnp.pad(rows, ((0, -rows.shape[0] % 8), (0, 0)))


def expert_rows(per_block):
    place = (jnp.arange(8) == lax.axis_index("expert")).astype(per_block.dtype)
    return per_block[:, None, :] * place[None, :, None]


def placed_weights(
    layer_input,
    output_grad,
    lengths,
    attn_routes,
    ffn_routes,
    norm1_gain,
    norm2_gain,
    attn_router,
    ffn_router,
    w_kv,
    w_query,
    w_out,
    w_in,
    w_down,
):
    f32, low = jnp.float32, jnp.bfloat16
    tokens, width = layer_input.shape[1:]
    experts = lax.axis_size("expert")
    contexts = lax.axis_size("context")
    slots = lax.axis_size("dp")
    shares = contexts * slots
    devices = experts * shares
    own_expert = lax.axis_index("expert")
    capacity = tokens * TOP // experts + tokens // 32
    room = -(-capacity // 8) * 8

    position = lax.axis_index(("expert", "context")) * tokens + jnp.arange(tokens, dtype=jnp.int32)
    live = (position < lengths[0]).astype(f32)
    x_float = layer_input[0].astype(f32)
    scale_one = rms_scale(x_float)
    normed_one = (x_float * scale_one * norm1_gain).astype(low)
    grad_out = output_grad[0].astype(f32) * live[:, None]

    shares_a, picked_a = pair_gates(
        jnp.dot(normed_one, attn_router, preferred_element_type=f32), attn_routes[0], live, experts
    )
    gates_a = jnp.sum(shares_a[:, :, None] * picked_a, axis=1)
    named_f = jnp.sum(
        (ffn_routes[0][:, :, None] == jnp.arange(experts, dtype=jnp.int32)).astype(f32), axis=1
    )
    named_f = named_f * live[:, None]
    all_one, aux, w_qkv = first_gather(
        [normed_one, as_rows(gates_a, named_f)], w_query[0], w_kv, 0
    )
    all_one, w_qkv = all_one.reshape(-1, width), w_qkv.reshape(width, -1)
    gate_a = lax.dynamic_index_in_dim(aux, own_expert, axis=1, keepdims=False)
    named = lax.dynamic_index_in_dim(aux, experts + own_expert, axis=1, keepdims=False)
    all_one, own_in = lax.optimization_barrier((all_one, w_in[0]))
    w_pair = lax.all_to_all(own_in, "context", split_axis=0, concat_axis=0, tiled=True)
    qkv = jnp.dot(all_one, w_qkv, preferred_element_type=f32).astype(low)
    attended, lse = attend(qkv, slots)
    gated = (attended.astype(f32) * gate_a.reshape(-1, 1)).astype(low)
    h1_part = jnp.dot(gated, w_out[0], preferred_element_type=f32).astype(low)
    (h1_sum,) = scatter_all([h1_part.reshape(devices, tokens, width)], 1)
    residual_one = x_float + h1_sum.astype(f32)

    scale_two = rms_scale(residual_one)
    normed_two = (residual_one * scale_two * norm2_gain).astype(low)
    shares_f, picked_f = pair_gates(
        jnp.dot(normed_two, ffn_router, preferred_element_type=f32), ffn_routes[0], live, experts
    )
    gates_f = jnp.sum(shares_f[:, :, None] * picked_f, axis=1)
    all_two, aux = gather_all([normed_two, as_rows(gates_f)], 2)
    gate_f = lax.dynamic_index_in_dim(aux, own_expert, axis=1, keepdims=False)
    all_two, grad_low = lax.optimization_barrier((all_two, grad_out.astype(low)))
    (all_grad,) = gather_all([grad_low], 7)
    all_grad, own_down = lax.optimization_barrier((all_grad, w_down[0]))
    share = lax.axis_index(SHARE)
    moves = [(s, (s % contexts) * slots + s // contexts) for s in range(shares)]
    stays = functools.reduce(jnp.logical_or, [share == s for s, d in moves if s == d])
    w_unit = lax.ppermute(own_down, SHARE, [(s, d) for s, d in moves if s != d])
    w_unit = jnp.where(stays, own_down, w_unit)
    units = w_unit.shape[0]
    earlier = (jnp.arange(tokens)[:, None] < jnp.arange(tokens)[None, :]).astype(f32)
    rank = jnp.dot(named, earlier, preferred_element_type=f32)
    table = jnp.where(
        rank[:, None, :] == jnp.arange(room, dtype=f32)[None, :, None], named[:, None, :], 0.0
    )
    low_table = table.astype(low)

    def pick(whole):
        rows = jnp.einsum(
            "bst,btd->bsd",
            low_table,
            whole,
            preferred_element_type=f32,
        )
        return rows.astype(low).reshape(devices * room, width)

    def put(rows):
        whole = jnp.einsum(
            "bst,bsd->btd", low_table, rows.reshape(devices, room, width), preferred_element_type=f32
        )
        return whole.astype(low)

    row_gate = jnp.sum(table * gate_f[:, None, :], axis=2).reshape(-1, 1)
    routed = pick(all_two)
    both = lax.dot_general(
        routed, w_pair, (((1,), (1,)), ((), ())), preferred_element_type=f32
    )
    gate_part, up_part = both[:, :units], both[:, units:]
    sigmoid_gate = jax.nn.sigmoid(gate_part)
    hidden_f = gate_part * sigmoid_gate * up_part
    hidden = hidden_f.astype(low)
    down = (jnp.dot(hidden, w_unit, preferred_element_type=f32) * row_gate).astype(low)
    d_rows = pick(all_grad)
    d_plain = lax.dot_general(d_rows, w_unit, (((1,), (1,)), ((), ())), preferred_element_type=f32)
    row_sums = jnp.sum(d_plain * hidden.astype(f32), axis=1).reshape(devices, room)
    dgate_part = expert_rows(jnp.sum(table * row_sums[:, :, None], axis=1))
    d_hidden = d_plain * row_gate
    d_gate = d_hidden * up_part * sigmoid_gate * (1.0 + gate_part * (1.0 - sigmoid_gate))
    d_up = d_hidden * gate_part * sigmoid_gate
    d_both = jnp.concatenate([d_gate, d_up], axis=1).astype(low)
    d_rows_two = jnp.dot(d_both, w_pair, preferred_element_type=f32).astype(low)
    d_two_part = put(d_rows_two)
    grad_unit = lax.dot_general(
        (hidden.astype(f32) * row_gate).astype(low),
        d_rows,
        (((0,), (0,)), ((), ())),
        preferred_element_type=f32,
    )
    grad_pair = lax.dot_general(
        d_both, routed, (((0,), (0,)), ((), ())), preferred_element_type=f32
    )
    mixed_part, d_two_part, grad_pair = lax.optimization_barrier(
        (put(down), d_two_part, grad_pair.astype(low))
    )
    (mixed,) = scatter_all([mixed_part], 3)
    layer_output = (live[:, None] * (residual_one + mixed.astype(f32))).astype(low)
    grad_unit = grad_unit.astype(low)
    grad_moved = lax.ppermute(grad_unit, SHARE, [(d, s) for s, d in moves if s != d])
    grad_w_down = jnp.where(stays, grad_unit, grad_moved).astype(f32)
    d_two_sum, dgate_f = scatter_all([d_two_part, dgate_part], 4)
    dgate_f = dgate_f[:experts].T
    dlog_f = gates_f * (dgate_f - jnp.sum(gates_f * dgate_f, axis=1, keepdims=True))
    d_normed_two = d_two_sum.astype(f32) + jnp.dot(
        dlog_f, ffn_router.astype(f32).T, precision=PRECISE
    )
    local_ffn_router = jnp.dot(dlog_f.T, normed_two.astype(f32), precision=PRECISE)
    d_mid, local_gain_two = norm_back(residual_one, scale_two, norm2_gain, d_normed_two)
    d_residual = grad_out + d_mid

    (all_mid,) = gather_all([d_residual.astype(low)], 5)
    all_mid = all_mid.reshape(-1, width)
    all_mid, grad_pair = lax.optimization_barrier((all_mid, grad_pair))
    grad_w_in = lax.all_to_all(grad_pair, "context", split_axis=0, concat_axis=0, tiled=True)
    grad_w_in = grad_w_in.astype(f32)
    d_att = lax.dot_general(
        all_mid, w_out[0], (((1,), (1,)), ((), ())), preferred_element_type=f32
    ).astype(low)
    d_qkv, head_sums = attend_back(qkv, d_att, lse, gate_a.reshape(slots, 1, -1), slots)
    grad_w_out = lax.dot_general(
        gated, all_mid, (((0,), (0,)), ((), ())), preferred_element_type=f32
    )
    dgate_part = expert_rows(jnp.sum(head_sums, axis=1).reshape(devices, tokens))
    d_one_part = lax.dot_general(
        d_qkv, w_qkv, (((1,), (1,)), ((), ())), preferred_element_type=f32
    ).astype(low)
    grad_qkv = lax.dot_general(
        all_one, d_qkv, (((0,), (0,)), ((), ())), preferred_element_type=f32
    ).astype(low)
    d_one_sum, dgate_a, grad_w_query, kv_grads = last_scatter(
        [d_one_part.reshape(devices, tokens, width), dgate_part],
        grad_qkv.reshape(shares, -1, w_qkv.shape[1]),
        6,
    )
    grad_w_query = grad_w_query.astype(f32)
    grad_w_kv = kv_grads.astype(f32)
    dgate_a = dgate_a[:experts].T
    dlog_a = gates_a * (dgate_a - jnp.sum(gates_a * dgate_a, axis=1, keepdims=True))
    d_normed_one = d_one_sum.astype(f32) + jnp.dot(
        dlog_a, attn_router.astype(f32).T, precision=PRECISE
    )
    local_attn_router = jnp.dot(dlog_a.T, normed_one.astype(f32), precision=PRECISE)
    d_first, local_gain_one = norm_back(x_float, scale_one, norm1_gain, d_normed_one)
    input_grad = d_residual + d_first
    sums = sum_all(
        jnp.concatenate(
            [local_gain_one[None], local_gain_two[None], local_attn_router, local_ffn_router]
        ).reshape(-1, HEAD_DIM),
        8,
    ).reshape(-1, width)
    gain_one_sum, gain_two_sum = sums[0], sums[1]
    router_a_sum, router_f_sum = sums[2 : 2 + experts].T, sums[2 + experts :].T
    return (
        layer_output[None],
        input_grad[None],
        gain_one_sum,
        gain_two_sum,
        router_a_sum,
        router_f_sum,
        grad_w_kv,
        grad_w_query[None],
        grad_w_out[None],
        grad_w_in[None],
        grad_w_down[None],
    )


def fits_in_place(mesh):
    sizes = (mesh.shape["expert"], mesh.shape["context"], mesh.shape["dp"])
    return sizes == (4, 2, 4)


def solution(mesh):
    placed = (
        P("dp", ("expert", "context"), None),
        P("dp", ("expert", "context"), None),
        P("dp"),
        P("dp", ("expert", "context"), None),
        P("dp", ("expert", "context"), None),
        P(),
        P(),
        P(),
        P(),
        P(("context", "dp"), None),
        P("expert", ("context", "dp"), None),
        P("expert", ("context", "dp"), None),
        P("expert", ("context", "dp"), None),
        P("expert", ("context", "dp"), None),
    )
    in_place = fits_in_place(mesh)
    return jax.shard_map(
        placed_weights if in_place else gathered_weights,
        mesh=mesh,
        in_specs=placed,
        out_specs=(
            P("dp", ("expert", "context"), None),
            P("dp", ("expert", "context"), None),
            P(),
            P(),
            P(),
            P(),
            P(("context", "dp"), None),
            P("expert", ("context", "dp"), None),
            P("expert", ("context", "dp"), None),
            P("expert", ("context", "dp"), None),
            P("expert", ("context", "dp"), None),
        ),
        check_vma=False,
    )
```
